512 devices in a mesh: role: 4 (over z_lo), tp: 4 (over x), dp: 32 (over y, z_hi, core).
Axes of the slice: x: 4, y: 4, z: 16 (z_hi: 4, z_lo: 4; z = z_hi * 4 + z_lo), core: 2. Of those that a mesh axis runs over, the one named last changes fastest.
Arguments:
- master: float32 [1024, 8192], P('tp', ('role', 'dp')), may hold values from -0.0625 to 0.0625
- key_bias: float32 [1024], P('tp'), may hold values from -3 to 3
- probe_tokens: bfloat16 [32768, 8192], P(('role', 'dp')), may hold values from -6 to 6
Outputs:
- weight: bfloat16 [8192, 1024], P(None, 'tp')
- probe_keys: bfloat16 [32768, 1024], P(('role', 'dp'), 'tp')
- checksum: float32 [8192], replicated
The draws below stay inside these ranges and needn't reach their ends.
All inputs are finite; a program needn't handle non-finite values.
Results may differ from the reference program's by a relative error of at most 0.005.
Values may be sent and summed in bfloat16 or wider, within the bound.
No kernel may reach another device: no remote copies, remote signals or barrier semaphores. Data moves between devices by JAX's collectives and lax.ppermute only.
A program may use at most 64 MiB of HBM per device.

```python
import jax
import jax.numpy as jnp

D = 8192
KVW = 1024
PROBES = 32768


def level_of(own_key, shape, cuts, least, largest):
    factor_of, own = 1.0, jax.random.fold_in(own_key, 6)
    for dim, parts in cuts:
        draws = jnp.exp(jax.random.uniform(jax.random.fold_in(own, dim), (parts,), jnp.float32, least / len(cuts), largest / len(cuts)))
        factor_of = factor_of * jnp.repeat(draws, shape[dim] // parts).reshape([-1 if axis == dim else 1 for axis in range(len(shape))])
    return factor_of


def bell_draw(stream_key, extent, scale, bound, pieces=(), kind=jnp.bfloat16):
    level = level_of(stream_key, extent, pieces, -0.22, 0.18) if pieces else 1.0
    values = jax.random.normal(stream_key, extent, jnp.float32) * scale * level
    return jnp.minimum(jnp.maximum(values, -bound), bound).astype(kind)


def setup_inputs(seed: int = 0) -> dict:
    keys = jax.random.split(jax.random.key(seed), 4)
    return {
        "master": bell_draw(keys[0], (KVW, D), D ** -0.5, 0.0625, ((0, 4), (1, 128)), jnp.float32),
        "key_bias": bell_draw(keys[1], (KVW,), 0.5, 3.0, ((0, 4),), jnp.float32),
        "probe_tokens": bell_draw(keys[2], (PROBES, D), 1.0, 6.0, ((0, 128),)),
    }


def reference(master, key_bias, probe_tokens):
    weight = jnp.transpose(master).astype(jnp.bfloat16)
    projected = jnp.dot(probe_tokens, weight, preferred_element_type=jnp.float32)
    probe_keys = (projected + key_bias[None, :]).astype(jnp.bfloat16)
    checksum = jnp.sum(weight.astype(jnp.float32), axis=1)
    return weight, probe_keys, checksum
```

```python
import itertools

import jax
import jax.numpy as jnp
from jax import lax
from jax.sharding import PartitionSpec as P

SIZES = {"y": 4, "z": 16, "core": 2}


def index_of(x, y, z, core):
    return ((z % 4) * 4 + x) * 32 + (y * 4 + z // 4) * 2 + core


PLANES = [
    [index_of(x, y, z, core) for y, z, core in itertools.product(range(4), range(16), range(2))]
    for x in range(4)
]


def over_copies(value, axis):
    copies = jnp.broadcast_to(value, (lax.axis_size(axis), *value.shape))
    return lax.all_to_all(copies, axis, split_axis=0, concat_axis=0, tiled=True).sum(axis=0)


def body(master, key_bias, probe_tokens):
    own_rows = jnp.transpose(master).astype(jnp.bfloat16)
    rows, heads = own_rows.shape
    plane = lax.all_gather(
        own_rows, ("role", "tp", "dp"), axis=0, tiled=True, axis_index_groups=PLANES
    )
    incoming = plane.reshape(4, 4, 4, 2 * rows, heads).transpose(2, 0, 1, 3, 4).reshape(-1, heads)
    totals = jnp.dot(probe_tokens, incoming, preferred_element_type=jnp.float32)
    probe_keys = (totals + key_bias[None, :]).astype(jnp.bfloat16)
    checksum = over_copies(jnp.sum(incoming.astype(jnp.float32), axis=1), "tp")
    return (incoming, probe_keys, checksum)


def solution(mesh):
    placed = (P("tp", ("role", "dp")), P("tp"), P(("role", "dp"), None))
    return jax.shard_map(
        body,
        mesh=mesh,
        in_specs=placed,
        out_specs=(P(None, "tp"), P(("role", "dp"), "tp"), P()),
        check_vma=False,
    )
```

```python
import functools
import itertools

import jax
import jax.numpy as jnp
from jax import lax
from jax.experimental import pallas as pl
from jax.experimental.pallas import tpu as pltpu
from jax.sharding import PartitionSpec as P


AXES = ("role", "tp", "dp")
NX, NY, NZ, NC, LO = 4, 4, 16, 2, 4
HI = NZ // LO
HALF = HI // 2


def index_of(x, y, z, core):
    y, z, core = y % NY, z % NZ, core % NC
    return ((z % LO) * NX + x) * (NY * HI * NC) + (y * HI + z // LO) * NC + core


CHIPS = list(itertools.product(range(NX), range(NY), range(NZ), range(NC)))
Z_RINGS = [
    [index_of(x, y, z, c) for z in range(NZ)]
    for x, y, c in itertools.product(range(NX), range(NY), range(NC))
]


def send_y(value, step):
    return lax.ppermute(
        value, AXES, [(index_of(x, y, z, c), index_of(x, y + step, z, c)) for x, y, z, c in CHIPS]
    )


def swap(value):
    return lax.ppermute(
        value, AXES, [(index_of(x, y, z, c), index_of(x, y, z, c + 1)) for x, y, z, c in CHIPS]
    )


def consume_kernel(units, first, last, n_before, rows, *refs):
    refs = list(refs)
    place = refs.pop(0)
    pieces = [(refs.pop(0), refs.pop(0)) for _ in units]
    probes = refs.pop(0)
    if not first:
        total_in, _ = refs.pop(0), refs.pop(0)
    before = [refs.pop(0) for _ in range(n_before)]
    if last:
        bias = refs.pop(0)
    weight, total_out, sums = refs.pop(0), refs.pop(0), refs.pop(0)
    block, cols, total, put_sem, get_sem = refs
    y, core = place[0], place[1]
    depth = HALF * NC * rows
    span = HI * NC * rows

    def row_of(rel, half, lo):
        return (lo * NY + lax.rem(y + rel, NY)) * span + half * depth

    gets = []
    for u, (rel, half) in enumerate(units):
        for lo in range(LO):
            at = pl.multiple_of(row_of(rel, half, lo), depth)
            get = pltpu.make_async_copy(
                probes.at[:, pl.ds(at, depth)], cols.at[u, lo], get_sem.at[u, lo]
            )
            get.start()
            gets.append(get)
    puts = []
    for u, (rel, half) in enumerate(units):
        for side, piece in enumerate(pieces[u]):
            of = core if side == 0 else 1 - core
            for k in range(HALF * LO):
                hi, lo = k // LO, k % LO
                at = row_of(rel, half, lo) + hi * NC * rows + of * rows
                put = pltpu.make_async_copy(
                    piece.at[pl.ds(k * rows, rows)],
                    weight.at[pl.ds(pl.multiple_of(at, rows), rows)],
                    put_sem,
                )
                put.start()
                puts.append(put)
                into = pl.multiple_of(hi * NC * rows + of * rows, rows)
                block[u, lo, pl.ds(into, rows), :] = piece[pl.ds(k * rows, rows), :]
    if first:
        total[...] = jnp.zeros_like(total)
    else:
        total[...] = total_in[...]
    ones = jnp.ones((8, block.shape[-1]), block.dtype)
    own_sums = []
    for u in range(len(units)):
        for lo in range(LO):
            w = block[u, lo]
            s = lax.dot_general(ones, w, (((1,), (1,)), ((), ())), preferred_element_type=jnp.float32)
            own_sums.append(s[0:1])
    for u in range(len(units)):
        for lo in range(LO):
            gets[u * LO + lo].wait()
            total[...] += jnp.dot(cols[u, lo], block[u, lo], preferred_element_type=jnp.float32)
    if last:
        done = [(ref, rel, half, u) for ref, us in zip(before, last) for u, (rel, half) in enumerate(us)]
        for ref, rel, half, u in done:
            for lo in range(LO):
                at = row_of(rel, half, lo) // depth
                for x in range(NX):
                    sums[x, pl.ds(at, 1), :] = ref[pl.ds(u * LO + lo, 1), :]
        for u, (rel, half) in enumerate(units):
            for lo in range(LO):
                at = row_of(rel, half, lo) // depth
                for x in range(NX):
                    sums[x, pl.ds(at, 1), :] = own_sums[u * LO + lo]
        total_out[...] = (total[...] + bias[...]).astype(total_out.dtype)
    else:
        for i, s in enumerate(own_sums):
            sums[i : i + 1, :] = s
        total_out[...] = total[...]
    for put in puts:
        put.wait()


def consume(place, units, pieces, probes, carried, bias=None, before=(), last=()):
    rows = pieces[0].shape[0] // (HALF * LO)
    heads = pieces[0].shape[1]
    tokens, width = probes.shape
    depth = HALF * NC * rows
    vmem = pl.BlockSpec(memory_space=pltpu.VMEM)
    hbm = pl.BlockSpec(memory_space=pl.ANY)
    smem = pl.BlockSpec(memory_space=pltpu.SMEM)
    first = carried is None
    operands = [place, *pieces, probes]
    specs = [smem, *[vmem] * len(pieces), hbm]
    aliases = {}
    if not first:
        aliases = {len(operands) + 1: 0}
        operands += [carried[1], carried[0]]
        specs += [vmem, hbm]
    operands += list(before)
    specs += [vmem] * len(before)
    if last:
        operands.append(bias.reshape(1, -1))
        specs.append(vmem)
        sums = jax.ShapeDtypeStruct((NX, width // depth, depth), jnp.float32)
    else:
        sums = jax.ShapeDtypeStruct((len(units) * LO, depth), jnp.float32)
    out_shape = (
        jax.ShapeDtypeStruct((width, heads), jnp.bfloat16),
        jax.ShapeDtypeStruct((tokens, heads), jnp.bfloat16 if last else jnp.float32),
        sums,
    )
    n = len(units)
    return pl.pallas_call(
        functools.partial(consume_kernel, units, first, last, len(before), rows),
        out_shape=out_shape,
        in_specs=specs,
        out_specs=(hbm, vmem, vmem),
        scratch_shapes=[
            pltpu.VMEM((n, LO, depth, heads), jnp.bfloat16),
            pltpu.VMEM((n, LO, tokens, depth), jnp.bfloat16),
            pltpu.VMEM((tokens, heads), jnp.float32),
            pltpu.SemaphoreType.DMA,
            pltpu.SemaphoreType.DMA((n, LO)),
        ],
        input_output_aliases=aliases,
        compiler_params=pltpu.CompilerParams(vmem_limit_bytes=(4 + 5 * n) << 20),
        cost_estimate=pl.CostEstimate(
            flops=2 * tokens * heads * depth * LO * n,
            bytes_accessed=2 * n * LO * depth * (heads + tokens),
            transcendentals=0,
        ),
    )(*operands)


def body(master, key_bias, probe_tokens):
    dp = lax.axis_index("dp")
    place = jnp.stack([lax.div(dp, HI * NC), lax.rem(dp, NC)])
    own_rows = jnp.transpose(master).astype(jnp.bfloat16)
    ring = lax.all_gather(own_rows, AXES, axis=0, tiled=True, axis_index_groups=Z_RINGS)
    half = ring.shape[0] // 2
    low, high = ring[:half], ring[half:]

    up_low = send_y(low, 1)
    down_high = send_y(high, -1)
    up_high = send_y(high, 1)
    down_low = send_y(low, -1)
    far_low = send_y(up_low, 1)
    far_high = send_y(down_high, -1)

    units_a = ((0, 0), (0, 1))
    pieces_a = [low, swap(low), high, swap(high)]
    a = consume(place, units_a, pieces_a, probe_tokens, None)
    units_b = ((3, 0), (1, 1), (3, 1), (1, 0))
    pieces_b = []
    for piece in (up_low, down_high, up_high, down_low):
        pieces_b += [piece, swap(piece)]
    b = consume(place, units_b, pieces_b, probe_tokens, a)
    units_c = ((2, 0), (2, 1))
    pieces_c = [far_low, swap(far_low), far_high, swap(far_high)]
    weight, probe_keys, sums = consume(
        place, units_c, pieces_c, probe_tokens, b, key_bias, (a[2], b[2]), (units_a, units_b)
    )
    gathered = lax.all_to_all(sums, "tp", split_axis=0, concat_axis=0, tiled=True)
    checksum = gathered.sum(axis=0).reshape(-1)
    return (weight, probe_keys, checksum)


def solution(mesh):
    placed = (P("tp", ("role", "dp")), P("tp"), P(("role", "dp"), None))
    return jax.shard_map(
        body,
        mesh=mesh,
        in_specs=placed,
        out_specs=(P(None, "tp"), P(("role", "dp"), "tp"), P()),
        check_vma=False,
    )
```

```python
import functools
import itertools

import jax
import jax.numpy as jnp
from jax import lax
from jax.experimental import pallas as pl
from jax.experimental.pallas import tpu as pltpu
from jax.sharding import PartitionSpec as P


AXES = ("role", "tp", "dp")
NX, NY, NZ, NC, LO = 4, 4, 16, 2, 4
HI = NZ // LO
LANES = 128
SAME, BACK, AHEAD, FAR = range(4)
CORE = 4


def index_of(x, y, z, core):
    y, z, core = y % NY, z % NZ, core % NC
    return ((z % LO) * NX + x) * (NY * HI * NC) + (y * HI + z // LO) * NC + core


CHIPS = list(itertools.product(range(NX), range(NY), range(NZ), range(NC)))
Z_RINGS = [
    [index_of(x, y, z, c) for z in range(NZ)]
    for x, y, c in itertools.product(range(NX), range(NY), range(NC))
]


ONWARD = [(index_of(x, y, z, c), index_of(x, y + 2 * c - 1, z, c)) for x, y, z, c in CHIPS]
SWAP = [(index_of(x, y, z, c), index_of(x, y, z, c + 1)) for x, y, z, c in CHIPS]


def onward(value):
    return lax.ppermute(value, AXES, ONWARD)


def swap(value):
    return lax.ppermute(value, AXES, SWAP)


def row_of(place, which, lo, span):
    return pl.multiple_of((lo * NY + place[which]) * span, span)


def fetch(place, which, probes, cols, sem):
    span = cols.shape[-1]
    gets = []
    for lo in range(LO):
        get = pltpu.make_async_copy(
            probes.at[:, pl.ds(row_of(place, which, lo, span), span)], cols.at[lo], sem.at[lo]
        )
        get.start()
        gets.append(get)
    return gets


def assemble(place, own, other, block, rows):
    for side, piece in enumerate((own, other)):
        core = place[CORE] if side == 0 else 1 - place[CORE]
        for z in range(NZ):
            into = pl.multiple_of(((z // LO) * NC + core) * rows, rows)
            block[z % LO, pl.ds(into, rows), :] = piece[pl.ds(z * rows, rows), :]


def row_sums(block):
    ones = jnp.ones((8, block.shape[-1]), block.dtype)
    return [
        lax.dot_general(
            ones, block[lo], (((1,), (1,)), ((), ())), preferred_element_type=jnp.float32
        )
        for lo in range(LO)
    ]


def step_kernel(which, rows, first, place, own, other, probes, *refs):
    if first:
        weight, total, sums, block, cols, put_sem, get_sem = refs
    else:
        total_in, _, weight, total, sums, block, cols, put_sem, get_sem = refs
    span = HI * NC * rows
    gets = fetch(place, which, probes, cols, get_sem)
    puts = []
    for side, piece in enumerate((own, other)):
        core = place[CORE] if side == 0 else 1 - place[CORE]
        for z in range(NZ):
            at = row_of(place, which, z % LO, span) + ((z // LO) * NC + core) * rows
            put = pltpu.make_async_copy(
                piece.at[pl.ds(z * rows, rows)],
                weight.at[pl.ds(pl.multiple_of(at, rows), rows)],
                put_sem,
            )
            put.start()
            puts.append(put)
    assemble(place, own, other, block, rows)
    for lo, s in enumerate(row_sums(block)):
        for j in range(span // LANES):
            sums[lo * (span // LANES) + j, :] = s[0, j * LANES : (j + 1) * LANES]
    acc = jnp.zeros(total.shape, total.dtype) if first else total_in[...]
    for lo in range(LO):
        gets[lo].wait()
        acc += jnp.dot(cols[lo], block[lo], preferred_element_type=jnp.float32)
    total[...] = acc
    for put in puts:
        put.wait()


def sums_kernel(rows, place, own, other, same, back, ahead, block, sums):
    span = HI * NC * rows
    lines = span // LANES
    assemble(place, own, other, block, rows)
    for which, ref in ((SAME, same), (BACK, back), (AHEAD, ahead)):
        for lo in range(LO):
            at = (lo * NY + place[which]) * lines
            for x in range(NX):
                sums[x, pl.ds(at, lines), :] = ref[lo * lines : (lo + 1) * lines, :]
    for lo, s in enumerate(row_sums(block)):
        at = (lo * NY + place[FAR]) * lines
        for x in range(NX):
            for j in range(lines):
                sums[x, pl.ds(at + j, 1), :] = s[0:1, j * LANES : (j + 1) * LANES]


def last_kernel(place, block, probes, total_in, bias, _, weight, keys, cols, put_sem, get_sem):
    span = block.shape[1]
    gets = fetch(place, FAR, probes, cols, get_sem)
    puts = []
    for lo in range(LO):
        put = pltpu.make_async_copy(
            block.at[lo], weight.at[pl.ds(row_of(place, FAR, lo, span), span)], put_sem.at[lo]
        )
        put.start()
        puts.append(put)
    acc = total_in[...] + bias[...]
    for lo in range(LO):
        gets[lo].wait()
        acc += jnp.dot(cols[lo], block[lo], preferred_element_type=jnp.float32)
    keys[...] = acc.astype(keys.dtype)
    for put in puts:
        put.wait()


VMEM = pl.BlockSpec(memory_space=pltpu.VMEM)
SMEM = pl.BlockSpec(memory_space=pltpu.SMEM)
HBM = pl.BlockSpec(memory_space=pltpu.HBM)
LIMIT = pltpu.CompilerParams(vmem_limit_bytes=50 << 20)


def sizes(piece, probes):
    rows = piece.shape[0] // NZ
    return rows, HI * NC * rows, piece.shape[1], probes.shape[0], probes.shape[1]


def cost(flops, moved):
    return pl.CostEstimate(flops=flops, bytes_accessed=moved, transcendentals=0)


def step(place, which, own, other, probes, carried=None):
    rows, span, heads, tokens, width = sizes(own, probes)
    first = carried is None
    return pl.pallas_call(
        functools.partial(step_kernel, which, rows, first),
        out_shape=(
            jax.ShapeDtypeStruct((width, heads), jnp.bfloat16),
            jax.ShapeDtypeStruct((tokens, heads), jnp.float32),
            jax.ShapeDtypeStruct((LO * span // LANES, LANES), jnp.float32),
        ),
        in_specs=[SMEM, VMEM, VMEM, HBM] + ([] if first else [VMEM, HBM]),
        out_specs=(HBM, VMEM, VMEM),
        scratch_shapes=[
            pltpu.VMEM((LO, span, heads), jnp.bfloat16),
            pltpu.VMEM((LO, tokens, span), jnp.bfloat16),
            pltpu.SemaphoreType.DMA,
            pltpu.SemaphoreType.DMA((LO,)),
        ],
        input_output_aliases={} if first else {5: 0},
        compiler_params=LIMIT,
        cost_estimate=cost(2 * LO * span * heads * tokens, 2 * LO * span * (heads + tokens)),
    )(place, own, other, probes, *(() if first else (carried[1], carried[0])))


def all_sums(place, own, other, probes, before):
    rows, span, heads, _, width = sizes(own, probes)
    return pl.pallas_call(
        functools.partial(sums_kernel, rows),
        out_shape=(
            jax.ShapeDtypeStruct((LO, span, heads), jnp.bfloat16),
            jax.ShapeDtypeStruct((NX, width // LANES, LANES), jnp.float32),
        ),
        in_specs=[SMEM] + [VMEM] * 5,
        out_specs=(VMEM, VMEM),
        compiler_params=LIMIT,
        cost_estimate=cost(2 * LO * span * heads * 8, 4 * LO * span * heads),
    )(place, own, other, *before)


def last(place, block, probes, carried, bias):
    _, span, heads = block.shape
    tokens, width = probes.shape
    return pl.pallas_call(
        last_kernel,
        out_shape=(
            jax.ShapeDtypeStruct((width, heads), jnp.bfloat16),
            jax.ShapeDtypeStruct((tokens, heads), jnp.bfloat16),
        ),
        in_specs=[SMEM, VMEM, HBM, VMEM, VMEM, HBM],
        out_specs=(HBM, VMEM),
        scratch_shapes=[
            pltpu.VMEM((LO, tokens, span), jnp.bfloat16),
            pltpu.SemaphoreType.DMA((LO,)),
            pltpu.SemaphoreType.DMA((LO,)),
        ],
        input_output_aliases={5: 0},
        compiler_params=LIMIT,
        cost_estimate=cost(2 * LO * span * heads * tokens, 2 * LO * span * (heads + tokens)),
    )(place, block, probes, carried[1], bias.reshape(1, -1), carried[0])


def body(master, key_bias, probe_tokens):
    dp = lax.axis_index("dp")
    core = lax.rem(dp, NC)
    y = lax.div(dp, HI * NC)
    back = lax.rem(y + 1 + 2 * core, NY)
    place = jnp.stack([y, back, lax.rem(back + 2, NY), lax.rem(y + 2, NY), core])

    own_rows = jnp.transpose(master).astype(jnp.bfloat16)
    mine = lax.all_gather(own_rows, AXES, axis=0, tiled=True, axis_index_groups=Z_RINGS)
    back_same = onward(mine)
    mine_other = swap(mine)
    back_other = onward(mine_other)
    far_same = onward(back_same)
    ahead_other = swap(back_same)
    ahead_same = swap(back_other)
    far_other = swap(far_same)

    s0 = step(place, SAME, mine, mine_other, probe_tokens)
    s1 = step(place, BACK, back_same, back_other, probe_tokens, s0)
    s2 = step(place, AHEAD, ahead_same, ahead_other, probe_tokens, s1)
    block, sums = all_sums(
        place, far_same, far_other, probe_tokens, (s0[2], s1[2], s2[2])
    )
    gathered = lax.all_to_all(sums, "tp", split_axis=0, concat_axis=0, tiled=True)
    weight, probe_keys = last(place, block, probe_tokens, s2, key_bias)
    checksum = gathered.sum(axis=0).reshape(-1)
    return (weight, probe_keys, checksum)


def solution(mesh):
    placed = (P("tp", ("role", "dp")), P("tp"), P(("role", "dp"), None))
    return jax.shard_map(
        body,
        mesh=mesh,
        in_specs=placed,
        out_specs=(P(None, "tp"), P(("role", "dp"), "tp"), P()),
        check_vma=False,
    )
```

```python
import functools
import itertools

import jax
import jax.numpy as jnp
from jax import lax
from jax.experimental import pallas as pl
from jax.experimental.pallas import tpu as pltpu
from jax.sharding import PartitionSpec as P


AXES = ("role", "tp", "dp")
NX, NY, NZ, NC, LO = 4, 4, 16, 2, 4
HI = NZ // LO
LANES = 128
SAME, BACK, AHEAD, FAR = range(4)
CORE = 4


def index_of(x, y, z, core):
    y, z, core = y % NY, z % NZ, core % NC
    return ((z % LO) * NX + x) * (NY * HI * NC) + (y * HI + z // LO) * NC + core


CHIPS = list(itertools.product(range(NX), range(NY), range(NZ), range(NC)))
Z_RINGS = [
    [index_of(x, y, z, c) for z in range(NZ)]
    for x, y, c in itertools.product(range(NX), range(NY), range(NC))
]


ONWARD = [(index_of(x, y, z, c), index_of(x, y + 2 * c - 1, z, c)) for x, y, z, c in CHIPS]
SWAP = [(index_of(x, y, z, c), index_of(x, y, z, c + 1)) for x, y, z, c in CHIPS]


def onward(value):
    return lax.ppermute(value, AXES, ONWARD)


def swap(value):
    return lax.ppermute(value, AXES, SWAP)


def row_of(place, which, lo, span):
    return pl.multiple_of((lo * NY + place[which]) * span, span)


def assemble(place, own, other, block, rows):
    for side, piece in enumerate((own, other)):
        core = place[CORE] if side == 0 else 1 - place[CORE]
        for z in range(NZ):
            into = pl.multiple_of(((z // LO) * NC + core) * rows, rows)
            block[z % LO, pl.ds(into, rows), :] = piece[pl.ds(z * rows, rows), :]


def row_sums(block):
    ones = jnp.ones((8, block.shape[-1]), block.dtype)
    return [
        lax.dot_general(
            ones, block[lo], (((1,), (1,)), ((), ())), preferred_element_type=jnp.float32
        )
        for lo in range(LO)
    ]


def put_rows(place, which, own, other, weight, rows, sem):
    span = HI * NC * rows
    puts = []
    for side, piece in enumerate((own, other)):
        core = place[CORE] if side == 0 else 1 - place[CORE]
        for z in range(NZ):
            at = row_of(place, which, z % LO, span) + ((z // LO) * NC + core) * rows
            put = pltpu.make_async_copy(
                piece.at[pl.ds(z * rows, rows)],
                weight.at[pl.ds(pl.multiple_of(at, rows), rows)],
                sem,
            )
            put.start()
            puts.append(put)
    return puts


def line_sums(block, sums):
    lines = block.shape[1] // LANES
    for lo, s in enumerate(row_sums(block)):
        for j in range(lines):
            sums[lo * lines + j, :] = s[0, j * LANES : (j + 1) * LANES]


def first_kernel(rows, place, own, other, probes, weight, total, sums, *refs):
    back, ahead, far, block, cols_same, put_sem, get_sem = refs
    cols = (cols_same, back, ahead, far)
    span = HI * NC * rows
    gets = []
    for which in range(NY):
        for lo in range(LO):
            get = pltpu.make_async_copy(
                probes.at[:, pl.ds(row_of(place, which, lo, span), span)],
                cols[which].at[lo],
                get_sem.at[which, lo],
            )
            get.start()
            gets.append(get)
    puts = put_rows(place, SAME, own, other, weight, rows, put_sem)
    assemble(place, own, other, block, rows)
    line_sums(block, sums)
    acc = jnp.zeros(total.shape, total.dtype)
    for lo in range(LO):
        gets[lo].wait()
        acc += jnp.dot(cols_same[lo], block[lo], preferred_element_type=jnp.float32)
    total[...] = acc
    for copy in puts + gets[LO:]:
        copy.wait()


def step_kernel(which, rows, place, own, other, cols, total_in, _, weight, total, sums, block, put_sem):
    puts = put_rows(place, which, own, other, weight, rows, put_sem)
    assemble(place, own, other, block, rows)
    acc = total_in[...]
    for lo in range(LO):
        acc += jnp.dot(cols[lo], block[lo], preferred_element_type=jnp.float32)
    total[...] = acc
    line_sums(block, sums)
    for put in puts:
        put.wait()


def sums_kernel(rows, place, own, other, same, back, ahead, block, sums):
    span = HI * NC * rows
    lines = span // LANES
    assemble(place, own, other, block, rows)
    for which, ref in ((SAME, same), (BACK, back), (AHEAD, ahead)):
        for lo in range(LO):
            at = (lo * NY + place[which]) * lines
            for x in range(NX):
                sums[x, pl.ds(at, lines), :] = ref[lo * lines : (lo + 1) * lines, :]
    for lo, s in enumerate(row_sums(block)):
        at = (lo * NY + place[FAR]) * lines
        for x in range(NX):
            for j in range(lines):
                sums[x, pl.ds(at + j, 1), :] = s[0:1, j * LANES : (j + 1) * LANES]


def last_kernel(place, block, cols, total_in, bias, _, weight, keys, put_sem):
    span = block.shape[1]
    part = span // HI
    puts = []
    for lo in range(LO):
        for hi in range(HI):
            at = row_of(place, FAR, lo, span) + hi * part
            put = pltpu.make_async_copy(
                block.at[lo, pl.ds(hi * part, part)],
                weight.at[pl.ds(pl.multiple_of(at, part), part)],
                put_sem,
            )
            put.start()
            puts.append(put)
    acc = total_in[...] + bias[...]
    for lo in range(LO):
        acc += jnp.dot(cols[lo], block[lo], preferred_element_type=jnp.float32)
    keys[...] = acc.astype(keys.dtype)
    for put in puts:
        put.wait()


VMEM = pl.BlockSpec(memory_space=pltpu.VMEM)
SMEM = pl.BlockSpec(memory_space=pltpu.SMEM)
HBM = pl.BlockSpec(memory_space=pltpu.HBM)
LIMIT = pltpu.CompilerParams(vmem_limit_bytes=46 << 20)


def sizes(piece, probes):
    rows = piece.shape[0] // NZ
    return rows, HI * NC * rows, piece.shape[1], probes.shape[0], probes.shape[1]


def cost(flops, moved):
    return pl.CostEstimate(flops=flops, bytes_accessed=moved, transcendentals=0)


def first_step(place, own, other, probes):
    rows, span, heads, tokens, width = sizes(own, probes)
    return pl.pallas_call(
        functools.partial(first_kernel, rows),
        out_shape=(
            jax.ShapeDtypeStruct((width, heads), jnp.bfloat16),
            jax.ShapeDtypeStruct((tokens, heads), jnp.float32),
            jax.ShapeDtypeStruct((LO * span // LANES, LANES), jnp.float32),
            *[jax.ShapeDtypeStruct((LO, tokens, span), jnp.bfloat16)] * 3,
        ),
        in_specs=[SMEM, VMEM, VMEM, HBM],
        out_specs=(HBM, *[VMEM] * 5),
        scratch_shapes=[
            pltpu.VMEM((LO, span, heads), jnp.bfloat16),
            pltpu.VMEM((LO, tokens, span), jnp.bfloat16),
            pltpu.SemaphoreType.DMA,
            pltpu.SemaphoreType.DMA((NY, LO)),
        ],
        compiler_params=LIMIT,
        cost_estimate=cost(2 * LO * span * heads * tokens, 2 * LO * span * (heads + NY * tokens)),
    )(place, own, other, probes)


def step(place, which, own, other, cols, carried):
    _, tokens, span = cols.shape
    width, heads = carried[0].shape
    rows = own.shape[0] // NZ
    return pl.pallas_call(
        functools.partial(step_kernel, which, rows),
        out_shape=(
            jax.ShapeDtypeStruct((width, heads), jnp.bfloat16),
            jax.ShapeDtypeStruct((tokens, heads), jnp.float32),
            jax.ShapeDtypeStruct((LO * span // LANES, LANES), jnp.float32),
        ),
        in_specs=[SMEM, VMEM, VMEM, VMEM, VMEM, HBM],
        out_specs=(HBM, VMEM, VMEM),
        scratch_shapes=[pltpu.VMEM((LO, span, heads), jnp.bfloat16), pltpu.SemaphoreType.DMA],
        input_output_aliases={5: 0},
        compiler_params=LIMIT,
        cost_estimate=cost(2 * LO * span * heads * tokens, 2 * LO * span * heads),
    )(place, own, other, cols, carried[1], carried[0])


def all_sums(place, own, other, probes, before):
    rows, span, heads, _, width = sizes(own, probes)
    return pl.pallas_call(
        functools.partial(sums_kernel, rows),
        out_shape=(
            jax.ShapeDtypeStruct((LO, span, heads), jnp.bfloat16),
            jax.ShapeDtypeStruct((NX, width // LANES, LANES), jnp.float32),
        ),
        in_specs=[SMEM] + [VMEM] * 5,
        out_specs=(VMEM, VMEM),
        compiler_params=LIMIT,
        cost_estimate=cost(2 * LO * span * heads * 8, 4 * LO * span * heads),
    )(place, own, other, *before)


def last(place, block, cols, carried, bias):
    _, span, heads = block.shape
    tokens, width = carried[1].shape[0], carried[0].shape[0]
    return pl.pallas_call(
        last_kernel,
        out_shape=(
            jax.ShapeDtypeStruct((width, heads), jnp.bfloat16),
            jax.ShapeDtypeStruct((tokens, heads), jnp.bfloat16),
        ),
        in_specs=[SMEM, VMEM, VMEM, VMEM, VMEM, HBM],
        out_specs=(HBM, VMEM),
        scratch_shapes=[pltpu.SemaphoreType.DMA],
        input_output_aliases={5: 0},
        compiler_params=LIMIT,
        cost_estimate=cost(2 * LO * span * heads * tokens, 2 * LO * span * heads),
    )(place, block, cols, carried[1], bias.reshape(1, -1), carried[0])


def body(master, key_bias, probe_tokens):
    dp = lax.axis_index("dp")
    core = lax.rem(dp, NC)
    y = lax.div(dp, HI * NC)
    back = lax.rem(y + 1 + 2 * core, NY)
    place = jnp.stack([y, back, lax.rem(back + 2, NY), lax.rem(y + 2, NY), core])

    own_rows = jnp.transpose(master).astype(jnp.bfloat16)
    mine = lax.all_gather(own_rows, AXES, axis=0, tiled=True, axis_index_groups=Z_RINGS)
    back_same = onward(mine)
    mine_other = swap(mine)
    back_other = onward(mine_other)
    far_same = onward(back_same)
    ahead_other = swap(back_same)
    ahead_same = swap(back_other)
    far_other = swap(far_same)

    *s0, cols_back, cols_ahead, cols_far = first_step(place, mine, mine_other, probe_tokens)
    s1 = step(place, BACK, back_same, back_other, cols_back, s0)
    s2 = step(place, AHEAD, ahead_same, ahead_other, cols_ahead, s1)
    block, sums = all_sums(
        place, far_same, far_other, probe_tokens, (s0[2], s1[2], s2[2])
    )
    gathered = lax.all_to_all(sums, "tp", split_axis=0, concat_axis=0, tiled=True)
    weight, probe_keys = last(place, block, cols_far, s2, key_bias)
    checksum = gathered.sum(axis=0).reshape(-1)
    return (weight, probe_keys, checksum)


def solution(mesh):
    placed = (P("tp", ("role", "dp")), P("tp"), P(("role", "dp"), None))
    return jax.shard_map(
        body,
        mesh=mesh,
        in_specs=placed,
        out_specs=(P(None, "tp"), P(("role", "dp"), "tp"), P()),
        check_vma=False,
    )
```

```python
import functools
import itertools

import jax
import jax.numpy as jnp
from jax import lax
from jax.experimental import pallas as pl
from jax.experimental.pallas import tpu as pltpu
from jax.sharding import PartitionSpec as P


AXES = ("role", "tp", "dp")
NX, NY, NZ, NC, LO = 4, 4, 16, 2, 4
HI = NZ // LO
LANES = 128
SAME, BACK, AHEAD, FAR = range(4)
CORE = 4


def index_of(x, y, z, core):
    y, z, core = y % NY, z % NZ, core % NC
    return ((z % LO) * NX + x) * (NY * HI * NC) + (y * HI + z // LO) * NC + core


CHIPS = list(itertools.product(range(NX), range(NY), range(NZ), range(NC)))
Z_RINGS = [
    [index_of(x, y, z, c) for z in range(NZ)]
    for x, y, c in itertools.product(range(NX), range(NY), range(NC))
]


ONWARD = [(index_of(x, y, z, c), index_of(x, y + 2 * c - 1, z, c)) for x, y, z, c in CHIPS]
TEAMS = [
    [index_of(x, y, z, c) for x, c in itertools.product(range(NX), range(NC))]
    for y, z in itertools.product(range(NY), range(NZ))
]
SWAP = [(index_of(x, y, z, c), index_of(x, y, z, c + 1)) for x, y, z, c in CHIPS]


def onward(value):
    return lax.ppermute(value, AXES, ONWARD)


def swap(value):
    return lax.ppermute(value, AXES, SWAP)


def row_of(place, which, lo, span):
    return pl.multiple_of((lo * NY + place[which]) * span, span)


def assemble(core, piece, block, rows):
    span = HI * NC * rows
    for z in range(NZ):
        at = (z % LO) * span + ((z // LO) * NC + core) * rows
        block[pl.ds(pl.multiple_of(at, rows), rows), :] = piece[pl.ds(z * rows, rows), :]


def row_sums(block):
    ones = jnp.ones((8, block.shape[-1]), block.dtype)
    return lax.dot_general(
        ones, block[...], (((1,), (1,)), ((), ())), preferred_element_type=jnp.float32
    )


def fetch(place, which, probes, cols, sem):
    span = cols.shape[1] // LO
    gets = []
    for lo in range(LO):
        get = pltpu.make_async_copy(
            probes.at[:, pl.ds(row_of(place, which, lo, span), span)],
            cols.at[:, pl.ds(lo * span, span)],
            sem,
        )
        get.start()
        gets.append(get)
    return gets


def put_rows(place, which, own, other, weight, rows, sem):
    span = HI * NC * rows
    puts = []
    for side, piece in enumerate((own, other)):
        core = place[CORE] if side == 0 else 1 - place[CORE]
        for z in range(NZ):
            at = row_of(place, which, z % LO, span) + ((z // LO) * NC + core) * rows
            put = pltpu.make_async_copy(
                piece.at[pl.ds(z * rows, rows)],
                weight.at[pl.ds(pl.multiple_of(at, rows), rows)],
                sem,
            )
            put.start()
            puts.append(put)
    return puts


def put_block(place, which, block, weight, rows, sem):
    span = HI * NC * rows
    part = NC * rows
    puts = []
    for lo in range(LO):
        for hi in range(HI):
            at = row_of(place, which, lo, span) + hi * part
            put = pltpu.make_async_copy(
                block.at[pl.ds(lo * span + hi * part, part)],
                weight.at[pl.ds(pl.multiple_of(at, part), part)],
                sem,
            )
            put.start()
            puts.append(put)
    return puts


def line_sums(block, sums):
    s = row_sums(block)
    for j in range(s.shape[1] // LANES):
        sums[j, :] = s[0, j * LANES : (j + 1) * LANES]


def first_kernel(rows, place, own, other, probes, weight, total, sums, *refs):
    cols_back, block, cols_same, put_sem, get_sem = refs
    gets = fetch(place, SAME, probes, cols_same, get_sem.at[0])
    gets += fetch(place, BACK, probes, cols_back, get_sem.at[1])
    puts = put_rows(place, SAME, own, other, weight, rows, put_sem)
    assemble(place[CORE], own, block, rows)
    assemble(1 - place[CORE], other, block, rows)
    line_sums(block, sums)
    for get in gets[:LO]:
        get.wait()
    total[...] = jnp.dot(cols_same[...], block[...], preferred_element_type=jnp.float32)
    for copy in puts + gets[LO:]:
        copy.wait()


def back_kernel(rows, place, own, other, cols, total_in, _, weight, total, sums, block, put_sem):
    puts = put_rows(place, BACK, own, other, weight, rows, put_sem)
    assemble(place[CORE], own, block, rows)
    assemble(1 - place[CORE], other, block, rows)
    line_sums(block, sums)
    total[...] = total_in[...] + jnp.dot(
        cols[...], block[...], preferred_element_type=jnp.float32
    )
    for put in puts:
        put.wait()


def ahead_kernel(rows, place, block, probes, total_in, _, weight, total, cols_far, cols, put_sem, get_sem):
    gets = fetch(place, AHEAD, probes, cols, get_sem.at[0])
    later = fetch(place, FAR, probes, cols_far, get_sem.at[1])
    puts = put_block(place, AHEAD, block, weight, rows, put_sem)
    for get in gets:
        get.wait()
    total[...] = total_in[...] + jnp.dot(
        cols[...], block[...], preferred_element_type=jnp.float32
    )
    for copy in puts + later:
        copy.wait()


def sums_kernel(rows, place, own, same, back, sums, block):
    lines = HI * NC * rows // LANES
    core = place[CORE]
    block[...] = jnp.zeros_like(block)
    assemble(core, own, block, rows)
    far = row_sums(block)
    own_part = same[...] * (core == 0).astype(jnp.float32)
    nothing = jnp.zeros((lines, LANES), jnp.float32)
    for copy in range(sums.shape[0]):
        for lo in range(LO):
            def put(which, value):
                sums[copy, pl.ds((lo * NY + place[which]) * lines, lines), :] = value

            put(SAME, own_part[lo * lines : (lo + 1) * lines, :])
            put(BACK, back[lo * lines : (lo + 1) * lines, :])
            put(AHEAD, nothing)
            for j in range(lines):
                at = (lo * lines + j) * LANES
                sums[copy, pl.ds((lo * NY + place[FAR]) * lines + j, 1), :] = far[0:1, at : at + LANES]


def last_kernel(rows, place, own, other, cols, total_in, bias, _, weight, keys, block, put_sem):
    puts = put_rows(place, FAR, own, other, weight, rows, put_sem)
    assemble(place[CORE], own, block, rows)
    assemble(1 - place[CORE], other, block, rows)
    total = total_in[...] + jnp.dot(cols[...], block[...], preferred_element_type=jnp.float32)
    keys[...] = (total + bias[...]).astype(keys.dtype)
    for put in puts:
        put.wait()


VMEM = pl.BlockSpec(memory_space=pltpu.VMEM)
SMEM = pl.BlockSpec(memory_space=pltpu.SMEM)
HBM = pl.BlockSpec(memory_space=pltpu.HBM)
LIMIT = pltpu.CompilerParams(vmem_limit_bytes=48 << 20)


def sizes(piece, probes):
    rows = piece.shape[0] // NZ
    return rows, HI * NC * rows, piece.shape[1], probes.shape[0], probes.shape[1]


def cost(flops, moved):
    return pl.CostEstimate(flops=flops, bytes_accessed=moved, transcendentals=0)


def first_step(place, own, other, probes):
    rows, span, heads, tokens, width = sizes(own, probes)
    depth = LO * span
    return pl.pallas_call(
        functools.partial(first_kernel, rows),
        out_shape=(
            jax.ShapeDtypeStruct((width, heads), jnp.bfloat16),
            jax.ShapeDtypeStruct((tokens, heads), jnp.float32),
            jax.ShapeDtypeStruct((depth // LANES, LANES), jnp.float32),
            jax.ShapeDtypeStruct((tokens, depth), jnp.bfloat16),
        ),
        in_specs=[SMEM, VMEM, VMEM, HBM],
        out_specs=(HBM, *[VMEM] * 3),
        scratch_shapes=[
            pltpu.VMEM((depth, heads), jnp.bfloat16),
            pltpu.VMEM((tokens, depth), jnp.bfloat16),
            pltpu.SemaphoreType.DMA,
            pltpu.SemaphoreType.DMA((2,)),
        ],
        compiler_params=LIMIT,
        cost_estimate=cost(2 * depth * heads * tokens, 2 * depth * (heads + 2 * tokens)),
    )(place, own, other, probes)


def back_step(place, own, other, cols, carried):
    tokens, depth = cols.shape
    width, heads = carried[0].shape
    return pl.pallas_call(
        functools.partial(back_kernel, own.shape[0] // NZ),
        out_shape=(
            jax.ShapeDtypeStruct((width, heads), jnp.bfloat16),
            jax.ShapeDtypeStruct((tokens, heads), jnp.float32),
            jax.ShapeDtypeStruct((depth // LANES, LANES), jnp.float32),
            jax.ShapeDtypeStruct((depth, heads), jnp.bfloat16),
        ),
        in_specs=[SMEM, VMEM, VMEM, VMEM, VMEM, HBM],
        out_specs=(HBM, VMEM, VMEM, VMEM),
        scratch_shapes=[pltpu.SemaphoreType.DMA],
        input_output_aliases={5: 0},
        compiler_params=LIMIT,
        cost_estimate=cost(2 * depth * heads * tokens, 2 * depth * heads),
    )(place, own, other, cols, carried[1], carried[0])


def ahead_step(place, block, probes, carried):
    depth, heads = block.shape
    tokens, width = probes.shape
    return pl.pallas_call(
        functools.partial(ahead_kernel, depth // (NZ * NC)),
        out_shape=(
            jax.ShapeDtypeStruct((width, heads), jnp.bfloat16),
            jax.ShapeDtypeStruct((tokens, heads), jnp.float32),
            jax.ShapeDtypeStruct((tokens, depth), jnp.bfloat16),
        ),
        in_specs=[SMEM, VMEM, HBM, VMEM, HBM],
        out_specs=(HBM, VMEM, VMEM),
        scratch_shapes=[
            pltpu.VMEM((tokens, depth), jnp.bfloat16),
            pltpu.SemaphoreType.DMA,
            pltpu.SemaphoreType.DMA((2,)),
        ],
        input_output_aliases={4: 0},
        compiler_params=LIMIT,
        cost_estimate=cost(2 * depth * heads * tokens, 2 * depth * (heads + 2 * tokens)),
    )(place, block, probes, carried[1], carried[0])


def team_sums(place, own, same, back, width):
    rows = own.shape[0] // NZ
    return pl.pallas_call(
        functools.partial(sums_kernel, rows),
        out_shape=jax.ShapeDtypeStruct((NX * NC, width // LANES, LANES), jnp.float32),
        in_specs=[SMEM] + [VMEM] * 3,
        out_specs=VMEM,
        scratch_shapes=[pltpu.VMEM((NC * own.shape[0], own.shape[1]), jnp.bfloat16)],
        compiler_params=LIMIT,
        cost_estimate=cost(16 * own.size * NC, 4 * own.size),
    )(place, own, same, back)


def last_step(place, own, other, cols, carried, bias):
    tokens, depth = cols.shape
    width, heads = carried[0].shape
    return pl.pallas_call(
        functools.partial(last_kernel, own.shape[0] // NZ),
        out_shape=(
            jax.ShapeDtypeStruct((width, heads), jnp.bfloat16),
            jax.ShapeDtypeStruct((tokens, heads), jnp.bfloat16),
        ),
        in_specs=[SMEM, VMEM, VMEM, VMEM, VMEM, VMEM, HBM],
        out_specs=(HBM, VMEM),
        scratch_shapes=[pltpu.VMEM((depth, heads), jnp.bfloat16), pltpu.SemaphoreType.DMA],
        input_output_aliases={6: 0},
        compiler_params=LIMIT,
        cost_estimate=cost(2 * depth * heads * tokens, 2 * depth * heads),
    )(place, own, other, cols, carried[1], bias.reshape(1, -1), carried[0])


def body(master, key_bias, probe_tokens):
    dp = lax.axis_index("dp")
    core = lax.rem(dp, NC)
    y = lax.div(dp, HI * NC)
    back = lax.rem(y + 1 + 2 * core, NY)
    place = jnp.stack([y, back, lax.rem(back + 2, NY), lax.rem(y + 2, NY), core])

    own_rows = jnp.transpose(master).astype(jnp.bfloat16)
    own_rows, place = lax.optimization_barrier((own_rows, place))
    mine = lax.all_gather(own_rows, AXES, axis=0, tiled=True, axis_index_groups=Z_RINGS)
    back_same = onward(mine)
    mine_other = swap(mine)
    back_other = onward(mine_other)
    far_same = onward(back_same)
    *s0, cols_back = first_step(place, mine, mine_other, probe_tokens)
    *s1, block = back_step(place, back_same, back_other, cols_back, s0)
    ahead = swap(block)
    sums = team_sums(place, far_same, s0[2], s1[2], probe_tokens.shape[1])
    gathered = lax.all_to_all(
        sums, AXES, split_axis=0, concat_axis=0, tiled=True, axis_index_groups=TEAMS
    )
    far_other = swap(far_same)
    *s2, cols_far = ahead_step(place, ahead, probe_tokens, s1)
    weight, probe_keys = last_step(place, far_same, far_other, cols_far, s2, key_bias)
    checksum = gathered.sum(axis=0).reshape(-1)
    return (weight, probe_keys, checksum)


def solution(mesh):
    placed = (P("tp", ("role", "dp")), P("tp"), P(("role", "dp"), None))
    return jax.shard_map(
        body,
        mesh=mesh,
        in_specs=placed,
        out_specs=(P(None, "tp"), P(("role", "dp"), "tp"), P()),
        check_vma=False,
    )
```

```python
import functools
import itertools

import jax
import jax.numpy as jnp
from jax import lax
from jax.experimental import pallas as pl
from jax.experimental.pallas import tpu as pltpu
from jax.sharding import PartitionSpec as P


AXES = ("role", "tp", "dp")
NX, NY, NZ, NC, LO = 4, 4, 16, 2, 4
HI = NZ // LO
LANES = 128
SAME, BACK, AHEAD, FAR = range(4)
CORE = 4


def index_of(x, y, z, core):
    y, z, core = y % NY, z % NZ, core % NC
    return ((z % LO) * NX + x) * (NY * HI * NC) + (y * HI + z // LO) * NC + core


CHIPS = list(itertools.product(range(NX), range(NY), range(NZ), range(NC)))
Z_RINGS = [
    [index_of(x, y, z, c) for z in range(NZ)]
    for x, y, c in itertools.product(range(NX), range(NY), range(NC))
]


ONWARD = [(index_of(x, y, z, c), index_of(x, y + 2 * c - 1, z, c)) for x, y, z, c in CHIPS]
CONTRARY = [(index_of(x, y, z, c), index_of(x, y + 1 - 2 * c, z, c)) for x, y, z, c in CHIPS]
TEAMS = [
    [index_of(x, y, z, c) for x, c in itertools.product(range(NX), range(NC))]
    for y, z in itertools.product(range(NY), range(NZ))
]
SWAP = [(index_of(x, y, z, c), index_of(x, y, z, c + 1)) for x, y, z, c in CHIPS]


def onward(value):
    return lax.ppermute(value, AXES, ONWARD)


def contrary(value):
    return lax.ppermute(value, AXES, CONTRARY)


def swap(value):
    return lax.ppermute(value, AXES, SWAP)


def row_of(place, which, lo, span):
    return pl.multiple_of((lo * NY + place[which]) * span, span)


def assemble(core, piece, block, rows):
    span = HI * NC * rows
    for z in range(NZ):
        at = (z % LO) * span + ((z // LO) * NC + core) * rows
        block[pl.ds(pl.multiple_of(at, rows), rows), :] = piece[pl.ds(z * rows, rows), :]


def row_sums(block):
    ones = jnp.ones((8, block.shape[-1]), block.dtype)
    return lax.dot_general(
        ones, block[...], (((1,), (1,)), ((), ())), preferred_element_type=jnp.float32
    )


def fetch(place, which, probes, cols, sem):
    span = cols.shape[1] // LO
    gets = []
    for lo in range(LO):
        get = pltpu.make_async_copy(
            probes.at[:, pl.ds(row_of(place, which, lo, span), span)],
            cols.at[:, pl.ds(lo * span, span)],
            sem,
        )
        get.start()
        gets.append(get)
    return gets


def put_rows(place, which, own, other, weight, rows, sem):
    span = HI * NC * rows
    puts = []
    for side, piece in enumerate((own, other)):
        core = place[CORE] if side == 0 else 1 - place[CORE]
        for z in range(NZ):
            at = row_of(place, which, z % LO, span) + ((z // LO) * NC + core) * rows
            put = pltpu.make_async_copy(
                piece.at[pl.ds(z * rows, rows)],
                weight.at[pl.ds(pl.multiple_of(at, rows), rows)],
                sem,
            )
            put.start()
            puts.append(put)
    return puts


def line_sums(block, sums, first):
    s = row_sums(block)
    for j in range(s.shape[1] // LANES):
        sums[first + j, :] = s[0, j * LANES : (j + 1) * LANES]


def near_kernel(rows, place, own, other, own_b, other_b, probes, weight, total, sums, *refs):
    blocks, cols, put_sem, get_sem = refs
    gets = [fetch(place, which, probes, cols.at[i], get_sem.at[i]) for i, which in enumerate((SAME, BACK))]
    puts = put_rows(place, SAME, own, other, weight, rows, put_sem)
    puts += put_rows(place, BACK, own_b, other_b, weight, rows, put_sem)
    core = place[CORE]
    for i, (mine, partner) in enumerate(((own, other), (own_b, other_b))):
        block = blocks.at[i]
        assemble(core, mine, block, rows)
        assemble(1 - core, partner, block, rows)
        line_sums(block, sums, i * (block.shape[0] // LANES))
    for i in range(2):
        for get in gets[i]:
            get.wait()
        part = jnp.dot(cols[i], blocks[i], preferred_element_type=jnp.float32)
        total[...] = part if i == 0 else total[...] + part
    for put in puts:
        put.wait()


def sums_kernel(rows, place, own, near, sums):
    lines = HI * NC * rows // LANES
    core = place[CORE]
    ones = jnp.ones((8, own.shape[1]), own.dtype)
    s = lax.dot_general(
        ones, own[...], (((1,), (1,)), ((), ())), preferred_element_type=jnp.float32
    )
    lane = lax.broadcasted_iota(jnp.int32, (1, LANES), 1)
    my_half = (lane // rows) == core
    own_part = near[: LO * lines, :] * (core == 0).astype(jnp.float32)
    nothing = jnp.zeros((lines, LANES), jnp.float32)
    for lo in range(LO):
        sums[0, pl.ds((lo * NY + place[SAME]) * lines, lines), :] = own_part[
            lo * lines : (lo + 1) * lines, :
        ]
        sums[0, pl.ds((lo * NY + place[BACK]) * lines, lines), :] = near[
            (LO + lo) * lines : (LO + lo + 1) * lines, :
        ]
        sums[0, pl.ds((lo * NY + place[AHEAD]) * lines, lines), :] = nothing
    for pair in range(NZ // 2):
        both = s[0:1, pair * LANES : (pair + 1) * LANES]
        turned = pltpu.roll(both, rows, 1)
        for odd in range(2):
            z = 2 * pair + odd
            line = jnp.where(core == odd, both, turned)
            at = (z % LO * NY + place[FAR]) * lines + z // LO
            sums[0, pl.ds(at, 1), :] = jnp.where(my_half, line, 0.0)
    whole = sums[0]
    for copy in range(1, sums.shape[0]):
        sums[copy] = whole


def last_kernel(rows, place, own, other, own_f, other_f, probes, total_in, bias, _, weight, keys, *refs):
    blocks, cols, put_sem, get_sem = refs
    gets = [fetch(place, which, probes, cols.at[i], get_sem.at[i]) for i, which in enumerate((AHEAD, FAR))]
    puts = put_rows(place, AHEAD, own, other, weight, rows, put_sem)
    puts += put_rows(place, FAR, own_f, other_f, weight, rows, put_sem)
    core = place[CORE]
    for i, (mine, partner) in enumerate(((own, other), (own_f, other_f))):
        assemble(core, mine, blocks.at[i], rows)
        assemble(1 - core, partner, blocks.at[i], rows)
    total = total_in[...] + bias[...]
    for i in range(2):
        for get in gets[i]:
            get.wait()
        total += jnp.dot(cols[i], blocks[i], preferred_element_type=jnp.float32)
    keys[...] = total.astype(keys.dtype)
    for put in puts:
        put.wait()


VMEM = pl.BlockSpec(memory_space=pltpu.VMEM)
SMEM = pl.BlockSpec(memory_space=pltpu.SMEM)
HBM = pl.BlockSpec(memory_space=pltpu.HBM)
LIMIT = pltpu.CompilerParams(vmem_limit_bytes=48 << 20)


def sizes(piece, probes):
    rows = piece.shape[0] // NZ
    return rows, HI * NC * rows, piece.shape[1], probes.shape[0], probes.shape[1]


def cost(flops, moved):
    return pl.CostEstimate(flops=flops, bytes_accessed=moved, transcendentals=0)


def scratch(tokens, depth, heads):
    return [
        pltpu.VMEM((2, depth, heads), jnp.bfloat16),
        pltpu.VMEM((2, tokens, depth), jnp.bfloat16),
        pltpu.SemaphoreType.DMA,
        pltpu.SemaphoreType.DMA((2,)),
    ]


def near_step(place, pieces, probes):
    rows, span, heads, tokens, width = sizes(pieces[0], probes)
    depth = LO * span
    return pl.pallas_call(
        functools.partial(near_kernel, rows),
        out_shape=(
            jax.ShapeDtypeStruct((width, heads), jnp.bfloat16),
            jax.ShapeDtypeStruct((tokens, heads), jnp.float32),
            jax.ShapeDtypeStruct((2 * depth // LANES, LANES), jnp.float32),
        ),
        in_specs=[SMEM, VMEM, VMEM, VMEM, VMEM, HBM],
        out_specs=(HBM, VMEM, VMEM),
        scratch_shapes=scratch(tokens, depth, heads),
        compiler_params=LIMIT,
        cost_estimate=cost(4 * depth * heads * tokens, 4 * depth * (heads + tokens)),
    )(place, *pieces, probes)


def team_sums(place, own, near, width):
    return pl.pallas_call(
        functools.partial(sums_kernel, own.shape[0] // NZ),
        out_shape=jax.ShapeDtypeStruct((NX * NC, width // LANES, LANES), jnp.float32),
        in_specs=[SMEM, VMEM, VMEM],
        out_specs=VMEM,
        compiler_params=LIMIT,
        cost_estimate=cost(16 * own.size, 2 * own.size),
    )(place, own, near)


def last_step(place, pieces, probes, carried, bias):
    rows, span, heads, tokens, width = sizes(pieces[0], probes)
    depth = LO * span
    return pl.pallas_call(
        functools.partial(last_kernel, rows),
        out_shape=(
            jax.ShapeDtypeStruct((width, heads), jnp.bfloat16),
            jax.ShapeDtypeStruct((tokens, heads), jnp.bfloat16),
        ),
        in_specs=[SMEM, VMEM, VMEM, VMEM, VMEM, HBM, VMEM, VMEM, HBM],
        out_specs=(HBM, VMEM),
        scratch_shapes=scratch(tokens, depth, heads),
        input_output_aliases={8: 0},
        compiler_params=LIMIT,
        cost_estimate=cost(4 * depth * heads * tokens, 4 * depth * (heads + tokens)),
    )(place, *pieces, probes, carried[1], bias.reshape(1, -1), carried[0])


def body(master, key_bias, probe_tokens):
    dp = lax.axis_index("dp")
    core = lax.rem(dp, NC)
    y = lax.div(dp, HI * NC)
    back = lax.rem(y + 1 + 2 * core, NY)
    place = jnp.stack([y, back, lax.rem(back + 2, NY), lax.rem(y + 2, NY), core])

    own_rows = jnp.transpose(master).astype(jnp.bfloat16)
    own_rows, place = lax.optimization_barrier((own_rows, place))
    mine = lax.all_gather(own_rows, AXES, axis=0, tiled=True, axis_index_groups=Z_RINGS)
    back = onward(mine)
    ahead = contrary(mine)
    far = onward(back)
    mine_other = swap(mine)
    ahead_other = swap(back)
    back_other = swap(ahead)
    far_other = swap(far)

    near = near_step(place, (mine, mine_other, back, back_other), probe_tokens)
    sums = team_sums(place, far, near[2], probe_tokens.shape[1])
    gathered = lax.all_to_all(
        sums, AXES, split_axis=0, concat_axis=0, tiled=True, axis_index_groups=TEAMS
    )
    weight, probe_keys = last_step(
        place, (ahead, ahead_other, far, far_other), probe_tokens, near, key_bias
    )
    checksum = gathered.sum(axis=0).reshape(-1)
    return (weight, probe_keys, checksum)


def solution(mesh):
    placed = (P("tp", ("role", "dp")), P("tp"), P(("role", "dp"), None))
    return jax.shard_map(
        body,
        mesh=mesh,
        in_specs=placed,
        out_specs=(P(None, "tp"), P(("role", "dp"), "tp"), P()),
        check_vma=False,
    )
```

```python
import functools
import itertools

import jax
import jax.numpy as jnp
from jax import lax
from jax.experimental import pallas as pl
from jax.experimental.pallas import tpu as pltpu
from jax.sharding import PartitionSpec as P


AXES = ("role", "tp", "dp")
NX, NY, NZ, NC, LO = 4, 4, 16, 2, 4
HI = NZ // LO
LANES = 128
SAME, BACK, AHEAD, FAR = range(4)
CORE = 4


def index_of(x, y, z, core):
    y, z, core = y % NY, z % NZ, core % NC
    return ((z % LO) * NX + x) * (NY * HI * NC) + (y * HI + z // LO) * NC + core


CHIPS = list(itertools.product(range(NX), range(NY), range(NZ), range(NC)))
Z_RINGS = [
    [index_of(x, y, z, c) for z in range(NZ)]
    for x, y, c in itertools.product(range(NX), range(NY), range(NC))
]


ONWARD = [(index_of(x, y, z, c), index_of(x, y + 2 * c - 1, z, c)) for x, y, z, c in CHIPS]
CONTRARY = [(index_of(x, y, z, c), index_of(x, y + 1 - 2 * c, z, c)) for x, y, z, c in CHIPS]
TEAMS = [
    [index_of(x, y, z, c) for x, c in itertools.product(range(NX), range(NC))]
    for y, z in itertools.product(range(NY), range(NZ))
]
SWAP = [(index_of(x, y, z, c), index_of(x, y, z, c + 1)) for x, y, z, c in CHIPS]


def onward(value):
    return lax.ppermute(value, AXES, ONWARD)


def contrary(value):
    return lax.ppermute(value, AXES, CONTRARY)


def swap(value):
    return lax.ppermute(value, AXES, SWAP)


def row_of(place, which, lo, span):
    return pl.multiple_of((lo * NY + place[which]) * span, span)


def assemble(core, piece, block, rows):
    span = HI * NC * rows
    for z in range(NZ):
        at = (z % LO) * span + ((z // LO) * NC + core) * rows
        block[pl.ds(pl.multiple_of(at, rows), rows), :] = piece[pl.ds(z * rows, rows), :]


def row_sums(block):
    ones = jnp.ones((8, block.shape[-1]), block.dtype)
    return lax.dot_general(
        ones, block[...], (((1,), (1,)), ((), ())), preferred_element_type=jnp.float32
    )


def fetch(place, which, probes, cols, sem):
    span = cols.shape[1] // LO
    gets = []
    for lo in range(LO):
        get = pltpu.make_async_copy(
            probes.at[:, pl.ds(row_of(place, which, lo, span), span)],
            cols.at[:, pl.ds(lo * span, span)],
            sem,
        )
        get.start()
        gets.append(get)
    return gets


def put_rows(place, which, own, other, weight, rows, sem):
    span = HI * NC * rows
    puts = []
    for side, piece in enumerate((own, other)):
        core = place[CORE] if side == 0 else 1 - place[CORE]
        for z in range(NZ):
            at = row_of(place, which, z % LO, span) + ((z // LO) * NC + core) * rows
            put = pltpu.make_async_copy(
                piece.at[pl.ds(z * rows, rows)],
                weight.at[pl.ds(pl.multiple_of(at, rows), rows)],
                sem,
            )
            put.start()
            puts.append(put)
    return puts


def line_sums(block, sums):
    s = row_sums(block)
    for j in range(s.shape[1] // LANES):
        sums[j, :] = s[0, j * LANES : (j + 1) * LANES]


def fetch_kernel(place, probes, same, back, sem):
    gets = []
    for which, cols in ((SAME, same), (BACK, back)):
        gets += fetch(place, which, probes, cols, sem)
    for get in gets:
        get.wait()


def near_kernel(which, rows, place, own, other, cols, *refs):
    total_in = None
    if which == SAME:
        weight, total, sums, block, put_sem = refs
    else:
        total_in, _, weight, total, sums, block, put_sem = refs
    puts = put_rows(place, which, own, other, weight, rows, put_sem)
    assemble(place[CORE], own, block, rows)
    assemble(1 - place[CORE], other, block, rows)
    line_sums(block, sums)
    part = jnp.dot(cols[...], block[...], preferred_element_type=jnp.float32)
    total[...] = part if total_in is None else total_in[...] + part
    for put in puts:
        put.wait()


def sums_kernel(rows, place, own, same, back, sums):
    lines = HI * NC * rows // LANES
    core = place[CORE]
    ones = jnp.ones((8, own.shape[1]), own.dtype)
    s = lax.dot_general(
        ones, own[...], (((1,), (1,)), ((), ())), preferred_element_type=jnp.float32
    )
    lane = lax.broadcasted_iota(jnp.int32, (1, LANES), 1)
    my_half = (lane // rows) == core
    own_part = same[...] * (core == 0).astype(jnp.float32)
    nothing = jnp.zeros((lines, LANES), jnp.float32)
    for lo in range(LO):
        sums[0, pl.ds((lo * NY + place[SAME]) * lines, lines), :] = own_part[
            lo * lines : (lo + 1) * lines, :
        ]
        sums[0, pl.ds((lo * NY + place[BACK]) * lines, lines), :] = back[
            lo * lines : (lo + 1) * lines, :
        ]
        sums[0, pl.ds((lo * NY + place[AHEAD]) * lines, lines), :] = nothing
    for pair in range(NZ // 2):
        both = s[0:1, pair * LANES : (pair + 1) * LANES]
        turned = pltpu.roll(both, rows, 1)
        for odd in range(2):
            z = 2 * pair + odd
            line = jnp.where(core == odd, both, turned)
            at = (z % LO * NY + place[FAR]) * lines + z // LO
            sums[0, pl.ds(at, 1), :] = jnp.where(my_half, line, 0.0)
    whole = sums[0]
    for copy in range(1, sums.shape[0]):
        sums[copy] = whole


def last_kernel(rows, place, own, other, own_f, other_f, probes, total_in, bias, _, weight, keys, *refs):
    blocks, cols, put_sem, get_sem = refs
    gets = [fetch(place, which, probes, cols.at[i], get_sem.at[i]) for i, which in enumerate((AHEAD, FAR))]
    puts = put_rows(place, AHEAD, own, other, weight, rows, put_sem)
    puts += put_rows(place, FAR, own_f, other_f, weight, rows, put_sem)
    core = place[CORE]
    for i, (mine, partner) in enumerate(((own, other), (own_f, other_f))):
        assemble(core, mine, blocks.at[i], rows)
        assemble(1 - core, partner, blocks.at[i], rows)
    total = total_in[...] + bias[...]
    for i in range(2):
        for get in gets[i]:
            get.wait()
        total += jnp.dot(cols[i], blocks[i], preferred_element_type=jnp.float32)
    keys[...] = total.astype(keys.dtype)
    for put in puts:
        put.wait()


VMEM = pl.BlockSpec(memory_space=pltpu.VMEM)
SMEM = pl.BlockSpec(memory_space=pltpu.SMEM)
HBM = pl.BlockSpec(memory_space=pltpu.HBM)
LIMIT = pltpu.CompilerParams(vmem_limit_bytes=49 << 20)
SMALL = pltpu.CompilerParams(vmem_limit_bytes=16 << 20)


def sizes(piece, probes):
    rows = piece.shape[0] // NZ
    return rows, HI * NC * rows, piece.shape[1], probes.shape[0], probes.shape[1]


def cost(flops, moved):
    return pl.CostEstimate(flops=flops, bytes_accessed=moved, transcendentals=0)


def fetch_step(place, probes, depth):
    tokens = probes.shape[0]
    return pl.pallas_call(
        fetch_kernel,
        out_shape=[jax.ShapeDtypeStruct((tokens, depth), jnp.bfloat16)] * 2,
        in_specs=[SMEM, HBM],
        out_specs=[VMEM] * 2,
        scratch_shapes=[pltpu.SemaphoreType.DMA],
        compiler_params=LIMIT,
        cost_estimate=cost(tokens * depth * 1000, 8 * tokens * depth),
    )(place, probes)


def near_step(place, which, own, other, cols, width, carried=None):
    tokens, depth = cols.shape
    heads = own.shape[1]
    first = carried is None
    return pl.pallas_call(
        functools.partial(near_kernel, which, own.shape[0] // NZ),
        out_shape=(
            jax.ShapeDtypeStruct((width, heads), jnp.bfloat16),
            jax.ShapeDtypeStruct((tokens, heads), jnp.float32),
            jax.ShapeDtypeStruct((depth // LANES, LANES), jnp.float32),
        ),
        in_specs=[SMEM, VMEM, VMEM, VMEM] + ([] if first else [VMEM, HBM]),
        out_specs=(HBM, VMEM, VMEM),
        scratch_shapes=[pltpu.VMEM((depth, heads), jnp.bfloat16), pltpu.SemaphoreType.DMA],
        input_output_aliases={} if first else {5: 0},
        compiler_params=SMALL,
        cost_estimate=cost(2 * depth * heads * tokens, 2 * depth * (heads + tokens)),
    )(place, own, other, cols, *(() if first else (carried[1], carried[0])))


def team_sums(place, own, same, back, width):
    return pl.pallas_call(
        functools.partial(sums_kernel, own.shape[0] // NZ),
        out_shape=jax.ShapeDtypeStruct((NX * NC, width // LANES, LANES), jnp.float32),
        in_specs=[SMEM, VMEM, VMEM, VMEM],
        out_specs=VMEM,
        compiler_params=SMALL,
        cost_estimate=cost(16 * own.size, 2 * own.size),
    )(place, own, same, back)


def last_step(place, pieces, probes, carried, bias):
    rows, span, heads, tokens, width = sizes(pieces[0], probes)
    depth = LO * span
    return pl.pallas_call(
        functools.partial(last_kernel, rows),
        out_shape=(
            jax.ShapeDtypeStruct((width, heads), jnp.bfloat16),
            jax.ShapeDtypeStruct((tokens, heads), jnp.bfloat16),
        ),
        in_specs=[SMEM, VMEM, VMEM, VMEM, VMEM, HBM, VMEM, VMEM, HBM],
        out_specs=(HBM, VMEM),
        scratch_shapes=[
            pltpu.VMEM((2, depth, heads), jnp.bfloat16),
            pltpu.VMEM((2, tokens, depth), jnp.bfloat16),
            pltpu.SemaphoreType.DMA,
            pltpu.SemaphoreType.DMA((2,)),
        ],
        input_output_aliases={8: 0},
        compiler_params=LIMIT,
        cost_estimate=cost(4 * depth * heads * tokens, 4 * depth * (heads + tokens)),
    )(place, *pieces, probes, carried[1], bias.reshape(1, -1), carried[0])


def body(master, key_bias, probe_tokens):
    dp = lax.axis_index("dp")
    core = lax.rem(dp, NC)
    y = lax.div(dp, HI * NC)
    back = lax.rem(y + 1 + 2 * core, NY)
    place = jnp.stack([y, back, lax.rem(back + 2, NY), lax.rem(y + 2, NY), core])

    own_rows = jnp.transpose(master).astype(jnp.bfloat16)
    own_rows, place = lax.optimization_barrier((own_rows, place))
    mine = lax.all_gather(own_rows, AXES, axis=0, tiled=True, axis_index_groups=Z_RINGS)
    back = onward(mine)
    ahead = contrary(mine)
    far = onward(back)
    mine_other = swap(mine)
    ahead_other = swap(back)
    back_other = swap(ahead)
    far_other = swap(far)

    width = probe_tokens.shape[1]
    cols = fetch_step(place, probe_tokens, 2 * mine.shape[0])
    s0 = near_step(place, SAME, mine, mine_other, cols[0], width)
    s1 = near_step(place, BACK, back, back_other, cols[1], width, s0)
    sums = team_sums(place, far, s0[2], s1[2], width)
    gathered = lax.all_to_all(
        sums, AXES, split_axis=0, concat_axis=0, tiled=True, axis_index_groups=TEAMS
    )
    weight, probe_keys = last_step(
        place, (ahead, ahead_other, far, far_other), probe_tokens, s1, key_bias
    )
    checksum = gathered.sum(axis=0).reshape(-1)
    return (weight, probe_keys, checksum)


def solution(mesh):
    placed = (P("tp", ("role", "dp")), P("tp"), P(("role", "dp"), None))
    return jax.shard_map(
        body,
        mesh=mesh,
        in_specs=placed,
        out_specs=(P(None, "tp"), P(("role", "dp"), "tp"), P()),
        check_vma=False,
    )
```

```python
import functools
import itertools

import jax
import jax.numpy as jnp
from jax import lax
from jax.experimental import pallas as pl
from jax.experimental.pallas import tpu as pltpu
from jax.sharding import PartitionSpec as P


AXES = ("role", "tp", "dp")
NX, NY, NZ, NC, LO = 4, 4, 16, 2, 4
HI = NZ // LO
LANES = 128
SAME, BACK, AHEAD, FAR = range(4)
CORE = 4


def index_of(x, y, z, core):
    y, z, core = y % NY, z % NZ, core % NC
    return ((z % LO) * NX + x) * (NY * HI * NC) + (y * HI + z // LO) * NC + core


CHIPS = list(itertools.product(range(NX), range(NY), range(NZ), range(NC)))
Z_RINGS = [
    [index_of(x, y, z, c) for z in range(NZ)]
    for x, y, c in itertools.product(range(NX), range(NY), range(NC))
]


ONWARD = [(index_of(x, y, z, c), index_of(x, y + 2 * c - 1, z, c)) for x, y, z, c in CHIPS]
TEAMS = [
    [index_of(x, y, z, c) for y, c in itertools.product(range(NY), range(NC))]
    for x, z in itertools.product(range(NX), range(NZ))
]
SWAP = [(index_of(x, y, z, c), index_of(x, y, z, c + 1)) for x, y, z, c in CHIPS]


def onward(value):
    return lax.ppermute(value, AXES, ONWARD)


def swap(value):
    return lax.ppermute(value, AXES, SWAP)


def row_of(place, which, lo, span):
    return pl.multiple_of((lo * NY + place[which]) * span, span)


def assemble(core, piece, block, rows):
    span = HI * NC * rows
    for z in range(NZ):
        at = (z % LO) * span + ((z // LO) * NC + core) * rows
        block[pl.ds(pl.multiple_of(at, rows), rows), :] = piece[pl.ds(z * rows, rows), :]


def fetch(place, which, probes, cols, sem):
    span = cols.shape[1] // LO
    gets = []
    for lo in range(LO):
        get = pltpu.make_async_copy(
            probes.at[:, pl.ds(row_of(place, which, lo, span), span)],
            cols.at[:, pl.ds(lo * span, span)],
            sem,
        )
        get.start()
        gets.append(get)
    return gets


def put_rows(place, which, own, other, weight, rows, sem):
    span = HI * NC * rows
    puts = []
    for side, piece in enumerate((own, other)):
        core = place[CORE] if side == 0 else 1 - place[CORE]
        for z in range(NZ):
            at = row_of(place, which, z % LO, span) + ((z // LO) * NC + core) * rows
            put = pltpu.make_async_copy(
                piece.at[pl.ds(z * rows, rows)],
                weight.at[pl.ds(pl.multiple_of(at, rows), rows)],
                sem,
            )
            put.start()
            puts.append(put)
    return puts


def put_block(place, which, block, weight, rows, sem):
    span = HI * NC * rows
    part = NC * rows
    puts = []
    for lo in range(LO):
        for hi in range(HI):
            at = row_of(place, which, lo, span) + hi * part
            put = pltpu.make_async_copy(
                block.at[pl.ds(lo * span + hi * part, part)],
                weight.at[pl.ds(pl.multiple_of(at, part), part)],
                sem,
            )
            put.start()
            puts.append(put)
    return puts


def sums_kernel(own, sums):
    ones = jnp.ones((8, own.shape[1]), own.dtype)
    s = lax.dot_general(
        ones, own[...], (((1,), (1,)), ((), ())), preferred_element_type=jnp.float32
    )
    for copy in range(NX):
        for j in range(s.shape[1] // LANES):
            sums[copy, j : j + 1, :] = s[0:1, j * LANES : (j + 1) * LANES]


def first_kernel(rows, place, own, other, probes, weight, total, cols, block, put_sem, get_sem):
    gets = fetch(place, SAME, probes, cols, get_sem)
    puts = put_rows(place, SAME, own, other, weight, rows, put_sem)
    assemble(place[CORE], own, block, rows)
    assemble(1 - place[CORE], other, block, rows)
    for get in gets:
        get.wait()
    total[...] = jnp.dot(cols[...], block[...], preferred_element_type=jnp.float32)
    for put in puts:
        put.wait()


def back_kernel(rows, place, own, other, probes, parts, total_in, _, weight, total, sums, block, *refs):
    cols, put_sem, get_sem = refs
    gets = fetch(place, BACK, probes, cols, get_sem)
    puts = put_rows(place, BACK, own, other, weight, rows, put_sem)
    assemble(place[CORE], own, block, rows)
    assemble(1 - place[CORE], other, block, rows)
    whole = parts[0]
    for x in range(1, NX):
        whole += parts[x]
    for copy in range(sums.shape[0]):
        sums[copy] = whole
    for get in gets:
        get.wait()
    total[...] = total_in[...] + jnp.dot(
        cols[...], block[...], preferred_element_type=jnp.float32
    )
    for put in puts:
        put.wait()


def ahead_kernel(rows, place, block, probes, total_in, _, weight, total, cols_far, cols, put_sem, get_sem):
    gets = fetch(place, AHEAD, probes, cols, get_sem.at[0])
    later = fetch(place, FAR, probes, cols_far, get_sem.at[1])
    puts = put_block(place, AHEAD, block, weight, rows, put_sem)
    for get in gets:
        get.wait()
    total[...] = total_in[...] + jnp.dot(
        cols[...], block[...], preferred_element_type=jnp.float32
    )
    for copy in puts + later:
        copy.wait()


def order_sums(sums, checksum, rows):
    first_half = lax.broadcasted_iota(jnp.int32, sums.shape[1:], 1) < rows
    for y in range(NY):
        zero, one = sums[y * NC], sums[y * NC + 1]
        lines = (
            jnp.where(first_half, zero, pltpu.roll(one, rows, 1)),
            jnp.where(first_half, pltpu.roll(zero, rows, 1), one),
        )
        for z in range(NZ):
            at = (z % LO * NY + y) * HI + z // LO
            checksum[at : at + 1, :] = lines[z % 2][z // 2 : z // 2 + 1, :]


def last_kernel(rows, place, own, other, cols, sums, total_in, bias, _, weight, keys, checksum, *refs):
    block, put_sem = refs
    puts = put_rows(place, FAR, own, other, weight, rows, put_sem)
    assemble(place[CORE], own, block, rows)
    assemble(1 - place[CORE], other, block, rows)
    total = total_in[...] + jnp.dot(cols[...], block[...], preferred_element_type=jnp.float32)
    keys[...] = (total + bias[...]).astype(keys.dtype)
    order_sums(sums, checksum, rows)
    for put in puts:
        put.wait()


VMEM = pl.BlockSpec(memory_space=pltpu.VMEM)
SMEM = pl.BlockSpec(memory_space=pltpu.SMEM)
HBM = pl.BlockSpec(memory_space=pltpu.HBM)
LIMIT = pltpu.CompilerParams(vmem_limit_bytes=50 << 20)
SMALL = pltpu.CompilerParams(vmem_limit_bytes=16 << 20)


def sizes(piece, probes):
    rows = piece.shape[0] // NZ
    return rows, HI * NC * rows, piece.shape[1], probes.shape[0], probes.shape[1]


def cost(flops, moved):
    return pl.CostEstimate(flops=flops, bytes_accessed=moved, transcendentals=0)


def own_sums(own):
    return pl.pallas_call(
        sums_kernel,
        out_shape=jax.ShapeDtypeStruct((NX, own.shape[0] // LANES, LANES), jnp.float32),
        in_specs=[VMEM],
        out_specs=VMEM,
        compiler_params=SMALL,
        cost_estimate=cost(16 * own.size, 2 * own.size),
    )(own)


def near_scratch(tokens, depth):
    return [
        pltpu.VMEM((tokens, depth), jnp.bfloat16),
        pltpu.SemaphoreType.DMA,
        pltpu.SemaphoreType.DMA,
    ]


def first_step(place, own, other, probes):
    rows, span, heads, tokens, width = sizes(own, probes)
    depth = LO * span
    cols, put_sem, get_sem = near_scratch(tokens, depth)
    return pl.pallas_call(
        functools.partial(first_kernel, rows),
        out_shape=(
            jax.ShapeDtypeStruct((width, heads), jnp.bfloat16),
            jax.ShapeDtypeStruct((tokens, heads), jnp.float32),
        ),
        in_specs=[SMEM, VMEM, VMEM, HBM],
        out_specs=(HBM, VMEM),
        scratch_shapes=[cols, pltpu.VMEM((depth, heads), jnp.bfloat16), put_sem, get_sem],
        compiler_params=LIMIT,
        cost_estimate=cost(2 * depth * heads * tokens, 2 * depth * (heads + tokens)),
    )(place, own, other, probes)


def back_step(place, own, other, probes, parts, carried):
    rows, span, heads, tokens, width = sizes(own, probes)
    depth = LO * span
    return pl.pallas_call(
        functools.partial(back_kernel, rows),
        out_shape=(
            jax.ShapeDtypeStruct((width, heads), jnp.bfloat16),
            jax.ShapeDtypeStruct((tokens, heads), jnp.float32),
            jax.ShapeDtypeStruct((NY * NC, *parts.shape[1:]), jnp.float32),
            jax.ShapeDtypeStruct((depth, heads), jnp.bfloat16),
        ),
        in_specs=[SMEM, VMEM, VMEM, HBM, VMEM, VMEM, HBM],
        out_specs=(HBM, VMEM, VMEM, VMEM),
        scratch_shapes=near_scratch(tokens, depth),
        input_output_aliases={6: 0},
        compiler_params=LIMIT,
        cost_estimate=cost(2 * depth * heads * tokens, 2 * depth * (heads + tokens)),
    )(place, own, other, probes, parts, carried[1], carried[0])


def ahead_step(place, block, probes, carried):
    depth, heads = block.shape
    tokens, width = probes.shape
    return pl.pallas_call(
        functools.partial(ahead_kernel, depth // (NZ * NC)),
        out_shape=(
            jax.ShapeDtypeStruct((width, heads), jnp.bfloat16),
            jax.ShapeDtypeStruct((tokens, heads), jnp.float32),
            jax.ShapeDtypeStruct((tokens, depth), jnp.bfloat16),
        ),
        in_specs=[SMEM, VMEM, HBM, VMEM, HBM],
        out_specs=(HBM, VMEM, VMEM),
        scratch_shapes=[
            pltpu.VMEM((tokens, depth), jnp.bfloat16),
            pltpu.SemaphoreType.DMA,
            pltpu.SemaphoreType.DMA((2,)),
        ],
        input_output_aliases={4: 0},
        compiler_params=LIMIT,
        cost_estimate=cost(2 * depth * heads * tokens, 2 * depth * (heads + 2 * tokens)),
    )(place, block, probes, carried[1], carried[0])


def last_step(place, own, other, cols, sums, carried, bias):
    tokens, depth = cols.shape
    width, heads = carried[0].shape
    return pl.pallas_call(
        functools.partial(last_kernel, own.shape[0] // NZ),
        out_shape=(
            jax.ShapeDtypeStruct((width, heads), jnp.bfloat16),
            jax.ShapeDtypeStruct((tokens, heads), jnp.bfloat16),
            jax.ShapeDtypeStruct((width // LANES, LANES), jnp.float32),
        ),
        in_specs=[SMEM, VMEM, VMEM, VMEM, VMEM, VMEM, VMEM, HBM],
        out_specs=(HBM, VMEM, VMEM),
        scratch_shapes=[pltpu.VMEM((depth, heads), jnp.bfloat16), pltpu.SemaphoreType.DMA],
        input_output_aliases={7: 0},
        compiler_params=SMALL,
        cost_estimate=cost(2 * depth * heads * tokens, 2 * depth * heads),
    )(place, own, other, cols, sums, carried[1], bias.reshape(1, -1), carried[0])


def body(master, key_bias, probe_tokens):
    dp = lax.axis_index("dp")
    core = lax.rem(dp, NC)
    y = lax.div(dp, HI * NC)
    back = lax.rem(y + 1 + 2 * core, NY)
    place = jnp.stack([y, back, lax.rem(back + 2, NY), lax.rem(y + 2, NY), core])

    own_rows = jnp.transpose(master).astype(jnp.bfloat16)
    own_rows, place = lax.optimization_barrier((own_rows, place))
    mine = lax.all_gather(own_rows, AXES, axis=0, tiled=True, axis_index_groups=Z_RINGS)
    back_same = onward(mine)
    mine_other = swap(mine)
    back_other = onward(mine_other)
    far_same = onward(back_same)
    own = own_sums(mine)
    parts = lax.all_to_all(own, "tp", split_axis=0, concat_axis=0, tiled=True)
    s0 = first_step(place, mine, mine_other, probe_tokens)
    *s1, totals, block = back_step(
        place, back_same, back_other, probe_tokens, parts, s0
    )
    ahead = swap(block)
    sums = lax.all_to_all(
        totals, AXES, split_axis=0, concat_axis=0, tiled=True, axis_index_groups=TEAMS
    )
    far_other = swap(far_same)
    *s2, cols_far = ahead_step(place, ahead, probe_tokens, s1)
    weight, probe_keys, checksum = last_step(
        place, far_same, far_other, cols_far, sums, s2, key_bias
    )
    checksum = checksum.reshape(-1)
    return (weight, probe_keys, checksum)


def solution(mesh):
    placed = (P("tp", ("role", "dp")), P("tp"), P(("role", "dp"), None))
    return jax.shard_map(
        body,
        mesh=mesh,
        in_specs=placed,
        out_specs=(P(None, "tp"), P(("role", "dp"), "tp"), P()),
        check_vma=False,
    )
```

```python
import functools
import itertools

import jax
import jax.numpy as jnp
from jax import lax
from jax.experimental import pallas as pl
from jax.experimental.pallas import tpu as pltpu
from jax.sharding import PartitionSpec as P


AXES = ("role", "tp", "dp")
NX, NY, NZ, NC, LO = 4, 4, 16, 2, 4
HI = NZ // LO
LANES = 128
SAME, BACK, AHEAD, FAR = range(4)
CORE = 4


def index_of(x, y, z, core):
    y, z, core = y % NY, z % NZ, core % NC
    return ((z % LO) * NX + x) * (NY * HI * NC) + (y * HI + z // LO) * NC + core


CHIPS = list(itertools.product(range(NX), range(NY), range(NZ), range(NC)))
Z_RINGS = [
    [index_of(x, y, z, c) for z in range(NZ)]
    for x, y, c in itertools.product(range(NX), range(NY), range(NC))
]


ONWARD = [(index_of(x, y, z, c), index_of(x, y + 2 * c - 1, z, c)) for x, y, z, c in CHIPS]
TEAMS = [
    [index_of(x, y, z, c) for y, c in itertools.product(range(NY), range(NC))]
    for x, z in itertools.product(range(NX), range(NZ))
]
SWAP = [(index_of(x, y, z, c), index_of(x, y, z, c + 1)) for x, y, z, c in CHIPS]


def onward(value):
    return lax.ppermute(value, AXES, ONWARD)


def swap(value):
    return lax.ppermute(value, AXES, SWAP)


def row_of(place, which, lo, span):
    return pl.multiple_of((lo * NY + place[which]) * span, span)


def assemble(core, piece, block, rows):
    span = HI * NC * rows
    for z in range(NZ):
        at = (z % LO) * span + ((z // LO) * NC + core) * rows
        block[pl.ds(pl.multiple_of(at, rows), rows), :] = piece[pl.ds(z * rows, rows), :]


def fetch(place, which, probes, cols, sem):
    span = cols.shape[1] // LO
    gets = []
    for lo in range(LO):
        get = pltpu.make_async_copy(
            probes.at[:, pl.ds(row_of(place, which, lo, span), span)],
            cols.at[:, pl.ds(lo * span, span)],
            sem,
        )
        get.start()
        gets.append(get)
    return gets


def put_rows(place, which, own, other, weight, rows, sem):
    span = HI * NC * rows
    puts = []
    for side, piece in enumerate((own, other)):
        core = place[CORE] if side == 0 else 1 - place[CORE]
        for z in range(NZ):
            at = row_of(place, which, z % LO, span) + ((z // LO) * NC + core) * rows
            put = pltpu.make_async_copy(
                piece.at[pl.ds(z * rows, rows)],
                weight.at[pl.ds(pl.multiple_of(at, rows), rows)],
                sem,
            )
            put.start()
            puts.append(put)
    return puts


def put_block(place, which, block, weight, rows, sem):
    span = HI * NC * rows
    part = NC * rows
    puts = []
    for lo in range(LO):
        for hi in range(HI):
            at = row_of(place, which, lo, span) + hi * part
            put = pltpu.make_async_copy(
                block.at[pl.ds(lo * span + hi * part, part)],
                weight.at[pl.ds(pl.multiple_of(at, part), part)],
                sem,
            )
            put.start()
            puts.append(put)
    return puts


def sums_kernel(own, sums):
    ones = jnp.ones((8, own.shape[1]), own.dtype)
    s = lax.dot_general(
        ones, own[...], (((1,), (1,)), ((), ())), preferred_element_type=jnp.float32
    )
    for copy in range(NX):
        for j in range(s.shape[1] // LANES):
            sums[copy, j : j + 1, :] = s[0:1, j * LANES : (j + 1) * LANES]


def first_kernel(rows, place, own, other, probes, weight, total, cols, block, put_sem, get_sem):
    gets = fetch(place, SAME, probes, cols, get_sem)
    puts = put_rows(place, SAME, own, other, weight, rows, put_sem)
    assemble(place[CORE], own, block, rows)
    assemble(1 - place[CORE], other, block, rows)
    for get in gets:
        get.wait()
    total[...] = jnp.dot(cols[...], block[...], preferred_element_type=jnp.float32)
    for put in puts:
        put.wait()


def back_kernel(rows, place, own, other, probes, parts, total_in, _, weight, total, sums, block, *refs):
    cols, put_sem, get_sem = refs
    gets = fetch(place, BACK, probes, cols, get_sem)
    puts = put_rows(place, BACK, own, other, weight, rows, put_sem)
    assemble(place[CORE], own, block, rows)
    assemble(1 - place[CORE], other, block, rows)
    whole = parts[0]
    for x in range(1, NX):
        whole += parts[x]
    for copy in range(sums.shape[0]):
        sums[copy] = whole
    for get in gets:
        get.wait()
    total[...] = total_in[...] + jnp.dot(
        cols[...], block[...], preferred_element_type=jnp.float32
    )
    for put in puts:
        put.wait()


def ahead_kernel(rows, place, block, probes, total_in, _, weight, total, cols_far, cols, put_sem, get_sem):
    gets = fetch(place, AHEAD, probes, cols, get_sem.at[0])
    later = fetch(place, FAR, probes, cols_far, get_sem.at[1])
    puts = put_block(place, AHEAD, block, weight, rows, put_sem)
    for get in gets:
        get.wait()
    total[...] = total_in[...] + jnp.dot(
        cols[...], block[...], preferred_element_type=jnp.float32
    )
    for copy in puts + later:
        copy.wait()


def order_kernel(rows, sums, checksum):
    first_half = lax.broadcasted_iota(jnp.int32, sums.shape[1:], 1) < rows
    for y in range(NY):
        zero, one = sums[y * NC], sums[y * NC + 1]
        lines = (
            jnp.where(first_half, zero, pltpu.roll(one, rows, 1)),
            jnp.where(first_half, pltpu.roll(zero, rows, 1), one),
        )
        for z in range(NZ):
            at = (z % LO * NY + y) * HI + z // LO
            checksum[at : at + 1, :] = lines[z % 2][z // 2 : z // 2 + 1, :]


def last_kernel(rows, place, own, other, cols, total_in, bias, _, weight, keys, block, put_sem):
    puts = put_rows(place, FAR, own, other, weight, rows, put_sem)
    assemble(place[CORE], own, block, rows)
    assemble(1 - place[CORE], other, block, rows)
    total = total_in[...] + jnp.dot(cols[...], block[...], preferred_element_type=jnp.float32)
    keys[...] = (total + bias[...]).astype(keys.dtype)
    for put in puts:
        put.wait()


VMEM = pl.BlockSpec(memory_space=pltpu.VMEM)
SMEM = pl.BlockSpec(memory_space=pltpu.SMEM)
HBM = pl.BlockSpec(memory_space=pltpu.HBM)
LIMIT = pltpu.CompilerParams(vmem_limit_bytes=50 << 20)
SMALL = pltpu.CompilerParams(vmem_limit_bytes=16 << 20)


def sizes(piece, probes):
    rows = piece.shape[0] // NZ
    return rows, HI * NC * rows, piece.shape[1], probes.shape[0], probes.shape[1]


def cost(flops, moved):
    return pl.CostEstimate(flops=flops, bytes_accessed=moved, transcendentals=0)


def own_sums(own):
    return pl.pallas_call(
        sums_kernel,
        out_shape=jax.ShapeDtypeStruct((NX, own.shape[0] // LANES, LANES), jnp.float32),
        in_specs=[VMEM],
        out_specs=VMEM,
        compiler_params=SMALL,
        cost_estimate=cost(16 * own.size, 2 * own.size),
    )(own)


def near_scratch(tokens, depth):
    return [
        pltpu.VMEM((tokens, depth), jnp.bfloat16),
        pltpu.SemaphoreType.DMA,
        pltpu.SemaphoreType.DMA,
    ]


def first_step(place, own, other, probes):
    rows, span, heads, tokens, width = sizes(own, probes)
    depth = LO * span
    cols, put_sem, get_sem = near_scratch(tokens, depth)
    return pl.pallas_call(
        functools.partial(first_kernel, rows),
        out_shape=(
            jax.ShapeDtypeStruct((width, heads), jnp.bfloat16),
            jax.ShapeDtypeStruct((tokens, heads), jnp.float32),
        ),
        in_specs=[SMEM, VMEM, VMEM, HBM],
        out_specs=(HBM, VMEM),
        scratch_shapes=[cols, pltpu.VMEM((depth, heads), jnp.bfloat16), put_sem, get_sem],
        compiler_params=LIMIT,
        cost_estimate=cost(2 * depth * heads * tokens, 2 * depth * (heads + tokens)),
    )(place, own, other, probes)


def back_step(place, own, other, probes, parts, carried):
    rows, span, heads, tokens, width = sizes(own, probes)
    depth = LO * span
    return pl.pallas_call(
        functools.partial(back_kernel, rows),
        out_shape=(
            jax.ShapeDtypeStruct((width, heads), jnp.bfloat16),
            jax.ShapeDtypeStruct((tokens, heads), jnp.float32),
            jax.ShapeDtypeStruct((NY * NC, *parts.shape[1:]), jnp.float32),
            jax.ShapeDtypeStruct((depth, heads), jnp.bfloat16),
        ),
        in_specs=[SMEM, VMEM, VMEM, HBM, VMEM, VMEM, HBM],
        out_specs=(HBM, VMEM, VMEM, VMEM),
        scratch_shapes=near_scratch(tokens, depth),
        input_output_aliases={6: 0},
        compiler_params=LIMIT,
        cost_estimate=cost(2 * depth * heads * tokens, 2 * depth * (heads + tokens)),
    )(place, own, other, probes, parts, carried[1], carried[0])


def ahead_step(place, block, probes, carried):
    depth, heads = block.shape
    tokens, width = probes.shape
    return pl.pallas_call(
        functools.partial(ahead_kernel, depth // (NZ * NC)),
        out_shape=(
            jax.ShapeDtypeStruct((width, heads), jnp.bfloat16),
            jax.ShapeDtypeStruct((tokens, heads), jnp.float32),
            jax.ShapeDtypeStruct((tokens, depth), jnp.bfloat16),
        ),
        in_specs=[SMEM, VMEM, HBM, VMEM, HBM],
        out_specs=(HBM, VMEM, VMEM),
        scratch_shapes=[
            pltpu.VMEM((tokens, depth), jnp.bfloat16),
            pltpu.SemaphoreType.DMA,
            pltpu.SemaphoreType.DMA((2,)),
        ],
        input_output_aliases={4: 0},
        compiler_params=LIMIT,
        cost_estimate=cost(2 * depth * heads * tokens, 2 * depth * (heads + 2 * tokens)),
    )(place, block, probes, carried[1], carried[0])


def order_sums(sums, rows):
    return pl.pallas_call(
        functools.partial(order_kernel, rows),
        out_shape=jax.ShapeDtypeStruct((sums.size // LANES, LANES), jnp.float32),
        in_specs=[VMEM],
        out_specs=VMEM,
        compiler_params=SMALL,
        cost_estimate=cost(sums.size, 8 * sums.size),
    )(sums)


def last_step(place, own, other, cols, carried, bias):
    tokens, depth = cols.shape
    width, heads = carried[0].shape
    return pl.pallas_call(
        functools.partial(last_kernel, own.shape[0] // NZ),
        out_shape=(
            jax.ShapeDtypeStruct((width, heads), jnp.bfloat16),
            jax.ShapeDtypeStruct((tokens, heads), jnp.bfloat16),
        ),
        in_specs=[SMEM, VMEM, VMEM, VMEM, VMEM, VMEM, HBM],
        out_specs=(HBM, VMEM),
        scratch_shapes=[pltpu.VMEM((depth, heads), jnp.bfloat16), pltpu.SemaphoreType.DMA],
        input_output_aliases={6: 0},
        compiler_params=SMALL,
        cost_estimate=cost(2 * depth * heads * tokens, 2 * depth * heads),
    )(place, own, other, cols, carried[1], bias.reshape(1, -1), carried[0])


def body(master, key_bias, probe_tokens):
    dp = lax.axis_index("dp")
    core = lax.rem(dp, NC)
    y = lax.div(dp, HI * NC)
    back = lax.rem(y + 1 + 2 * core, NY)
    place = jnp.stack([y, back, lax.rem(back + 2, NY), lax.rem(y + 2, NY), core])

    own_rows = jnp.transpose(master).astype(jnp.bfloat16)
    own_rows, place = lax.optimization_barrier((own_rows, place))
    mine = lax.all_gather(own_rows, AXES, axis=0, tiled=True, axis_index_groups=Z_RINGS)
    back_same = onward(mine)
    mine_other = swap(mine)
    back_other = onward(mine_other)
    far_same = onward(back_same)
    own = own_sums(mine)
    parts = lax.all_to_all(own, "tp", split_axis=0, concat_axis=0, tiled=True)
    s0 = first_step(place, mine, mine_other, probe_tokens)
    *s1, totals, block = back_step(
        place, back_same, back_other, probe_tokens, parts, s0
    )
    ahead = swap(block)
    sums = lax.all_to_all(
        totals, AXES, split_axis=0, concat_axis=0, tiled=True, axis_index_groups=TEAMS
    )
    far_other = swap(far_same)
    *s2, cols_far = ahead_step(place, ahead, probe_tokens, s1)
    weight, probe_keys = last_step(place, far_same, far_other, cols_far, s2, key_bias)
    checksum = order_sums(sums, own_rows.shape[0]).reshape(-1)
    return (weight, probe_keys, checksum)


def solution(mesh):
    placed = (P("tp", ("role", "dp")), P("tp"), P(("role", "dp"), None))
    return jax.shard_map(
        body,
        mesh=mesh,
        in_specs=placed,
        out_specs=(P(None, "tp"), P(("role", "dp"), "tp"), P()),
        check_vma=False,
    )
```

```python
import functools
import itertools

import jax
import jax.numpy as jnp
from jax import lax
from jax.experimental import pallas as pl
from jax.experimental.pallas import tpu as pltpu
from jax.sharding import PartitionSpec as P


AXES = ("role", "tp", "dp")
NX, NY, NZ, NC, LO = 4, 4, 16, 2, 4
HI = NZ // LO
LANES = 128
SAME, BACK, AHEAD, FAR = range(4)
CORE = 4


def index_of(x, y, z, core):
    y, z, core = y % NY, z % NZ, core % NC
    return ((z % LO) * NX + x) * (NY * HI * NC) + (y * HI + z // LO) * NC + core


CHIPS = list(itertools.product(range(NX), range(NY), range(NZ), range(NC)))
Z_RINGS = [
    [index_of(x, y, z, c) for z in range(NZ)]
    for x, y, c in itertools.product(range(NX), range(NY), range(NC))
]


ONWARD = [(index_of(x, y, z, c), index_of(x, y + 2 * c - 1, z, c)) for x, y, z, c in CHIPS]
TEAMS = [
    [index_of(x, y, z, c) for y, c in itertools.product(range(NY), range(NC))]
    for x, z in itertools.product(range(NX), range(NZ))
]
SWAP = [(index_of(x, y, z, c), index_of(x, y, z, c + 1)) for x, y, z, c in CHIPS]


def onward(value):
    return lax.ppermute(value, AXES, ONWARD)


def swap(value):
    return lax.ppermute(value, AXES, SWAP)


def row_of(place, which, lo, span):
    return pl.multiple_of((lo * NY + place[which]) * span, span)


def assemble(core, piece, block, rows):
    span = HI * NC * rows
    for z in range(NZ):
        at = (z % LO) * span + ((z // LO) * NC + core) * rows
        block[pl.ds(pl.multiple_of(at, rows), rows), :] = piece[pl.ds(z * rows, rows), :]


def fetch(place, which, probes, cols, sem):
    span = cols.shape[1] // LO
    gets = []
    for lo in range(LO):
        get = pltpu.make_async_copy(
            probes.at[:, pl.ds(row_of(place, which, lo, span), span)],
            cols.at[:, pl.ds(lo * span, span)],
            sem,
        )
        get.start()
        gets.append(get)
    return gets


def put_rows(place, which, own, other, weight, rows, sem):
    span = HI * NC * rows
    puts = []
    for side, piece in enumerate((own, other)):
        core = place[CORE] if side == 0 else 1 - place[CORE]
        for z in range(NZ):
            at = row_of(place, which, z % LO, span) + ((z // LO) * NC + core) * rows
            put = pltpu.make_async_copy(
                piece.at[pl.ds(z * rows, rows)],
                weight.at[pl.ds(pl.multiple_of(at, rows), rows)],
                sem,
            )
            put.start()
            puts.append(put)
    return puts


def put_block(place, which, block, weight, rows, sem):
    span = HI * NC * rows
    part = NC * rows
    puts = []
    for lo in range(LO):
        for hi in range(HI):
            at = row_of(place, which, lo, span) + hi * part
            put = pltpu.make_async_copy(
                block.at[pl.ds(lo * span + hi * part, part)],
                weight.at[pl.ds(pl.multiple_of(at, part), part)],
                sem,
            )
            put.start()
            puts.append(put)
    return puts


def sums_kernel(own, sums):
    ones = jnp.ones((8, own.shape[1]), own.dtype)
    s = lax.dot_general(
        ones, own[...], (((1,), (1,)), ((), ())), preferred_element_type=jnp.float32
    )
    for copy in range(NX):
        for j in range(s.shape[1] // LANES):
            sums[copy, j : j + 1, :] = s[0:1, j * LANES : (j + 1) * LANES]


def first_kernel(rows, place, own, other, probes, weight, total, cols, block, put_sem, get_sem):
    gets = fetch(place, SAME, probes, cols, get_sem)
    puts = put_rows(place, SAME, own, other, weight, rows, put_sem)
    assemble(place[CORE], own, block, rows)
    assemble(1 - place[CORE], other, block, rows)
    for get in gets:
        get.wait()
    total[...] = jnp.dot(cols[...], block[...], preferred_element_type=jnp.float32)
    for put in puts:
        put.wait()


def block_kernel(rows, place, own, other, parts, totals, block, sums, sums_sem):
    whole = parts[0]
    for x in range(1, NX):
        whole += parts[x]
    for copy in range(sums.shape[0]):
        sums[copy] = whole
    assemble(place[CORE], own, block, rows)
    assemble(1 - place[CORE], other, block, rows)
    out = pltpu.make_async_copy(sums, totals, sums_sem)
    out.start()
    out.wait()


def back_kernel(rows, place, block, probes, total_in, _, weight, total, cols, put_sem, get_sem):
    gets = fetch(place, BACK, probes, cols, get_sem)
    puts = put_block(place, BACK, block, weight, rows, put_sem)
    for get in gets:
        get.wait()
    total[...] = total_in[...] + jnp.dot(
        cols[...], block[...], preferred_element_type=jnp.float32
    )
    for put in puts:
        put.wait()


def ahead_kernel(rows, place, block, probes, total_in, _, weight, total, cols_far, cols, put_sem, get_sem):
    gets = fetch(place, AHEAD, probes, cols, get_sem.at[0])
    later = fetch(place, FAR, probes, cols_far, get_sem.at[1])
    puts = put_block(place, AHEAD, block, weight, rows, put_sem)
    for get in gets:
        get.wait()
    total[...] = total_in[...] + jnp.dot(
        cols[...], block[...], preferred_element_type=jnp.float32
    )
    for copy in puts + later:
        copy.wait()


def order_kernel(rows, sums, checksum):
    first_half = lax.broadcasted_iota(jnp.int32, sums.shape[1:], 1) < rows
    for y in range(NY):
        zero, one = sums[y * NC], sums[y * NC + 1]
        lines = (
            jnp.where(first_half, zero, pltpu.roll(one, rows, 1)),
            jnp.where(first_half, pltpu.roll(zero, rows, 1), one),
        )
        for z in range(NZ):
            at = (z % LO * NY + y) * HI + z // LO
            checksum[at : at + 1, :] = lines[z % 2][z // 2 : z // 2 + 1, :]


def last_kernel(rows, place, own, other, cols, total_in, bias, _, weight, keys, block, made, put_sem, keys_sem):
    puts = put_rows(place, FAR, own, other, weight, rows, put_sem)
    assemble(place[CORE], own, block, rows)
    assemble(1 - place[CORE], other, block, rows)
    total = total_in[...] + jnp.dot(cols[...], block[...], preferred_element_type=jnp.float32)
    made[...] = (total + bias[...]).astype(made.dtype)
    for put in puts[: len(puts) // 2]:
        put.wait()
    out = pltpu.make_async_copy(made, keys, keys_sem)
    out.start()
    for copy in puts[len(puts) // 2 :] + [out]:
        copy.wait()


VMEM = pl.BlockSpec(memory_space=pltpu.VMEM)
SMEM = pl.BlockSpec(memory_space=pltpu.SMEM)
HBM = pl.BlockSpec(memory_space=pltpu.HBM)
LIMIT = pltpu.CompilerParams(vmem_limit_bytes=50 << 20)
SMALL = pltpu.CompilerParams(vmem_limit_bytes=16 << 20)


def sizes(piece, probes):
    rows = piece.shape[0] // NZ
    return rows, HI * NC * rows, piece.shape[1], probes.shape[0], probes.shape[1]


def cost(flops, moved):
    return pl.CostEstimate(flops=flops, bytes_accessed=moved, transcendentals=0)


def own_sums(own):
    return pl.pallas_call(
        sums_kernel,
        out_shape=jax.ShapeDtypeStruct((NX, own.shape[0] // LANES, LANES), jnp.float32),
        in_specs=[VMEM],
        out_specs=VMEM,
        compiler_params=SMALL,
        cost_estimate=cost(16 * own.size, 2 * own.size),
    )(own)


def near_scratch(tokens, depth):
    return [
        pltpu.VMEM((tokens, depth), jnp.bfloat16),
        pltpu.SemaphoreType.DMA,
        pltpu.SemaphoreType.DMA,
    ]


def first_step(place, own, other, probes):
    rows, span, heads, tokens, width = sizes(own, probes)
    depth = LO * span
    cols, put_sem, get_sem = near_scratch(tokens, depth)
    return pl.pallas_call(
        functools.partial(first_kernel, rows),
        out_shape=(
            jax.ShapeDtypeStruct((width, heads), jnp.bfloat16),
            jax.ShapeDtypeStruct((tokens, heads), jnp.float32),
        ),
        in_specs=[SMEM, VMEM, VMEM, HBM],
        out_specs=(HBM, VMEM),
        scratch_shapes=[cols, pltpu.VMEM((depth, heads), jnp.bfloat16), put_sem, get_sem],
        compiler_params=LIMIT,
        cost_estimate=cost(2 * depth * heads * tokens, 2 * depth * (heads + tokens)),
    )(place, own, other, probes)


def block_step(place, own, other, parts):
    rows, heads = own.shape[0] // NZ, own.shape[1]
    shape = (NY * NC, *parts.shape[1:])
    return pl.pallas_call(
        functools.partial(block_kernel, rows),
        out_shape=(
            jax.ShapeDtypeStruct(shape, jnp.float32),
            jax.ShapeDtypeStruct((NC * own.shape[0], heads), jnp.bfloat16),
        ),
        in_specs=[SMEM, VMEM, VMEM, VMEM],
        out_specs=(HBM, VMEM),
        scratch_shapes=[pltpu.VMEM(shape, jnp.float32), pltpu.SemaphoreType.DMA],
        compiler_params=SMALL,
        cost_estimate=cost(16 * own.size, 8 * own.size),
    )(place, own, other, parts)


def back_step(place, block, probes, carried):
    depth, heads = block.shape
    tokens, width = probes.shape
    return pl.pallas_call(
        functools.partial(back_kernel, depth // (NZ * NC)),
        out_shape=(
            jax.ShapeDtypeStruct((width, heads), jnp.bfloat16),
            jax.ShapeDtypeStruct((tokens, heads), jnp.float32),
        ),
        in_specs=[SMEM, VMEM, HBM, VMEM, HBM],
        out_specs=(HBM, VMEM),
        scratch_shapes=near_scratch(tokens, depth),
        input_output_aliases={4: 0},
        compiler_params=LIMIT,
        cost_estimate=cost(2 * depth * heads * tokens, 2 * depth * (heads + tokens)),
    )(place, block, probes, carried[1], carried[0])


def ahead_step(place, block, probes, carried):
    depth, heads = block.shape
    tokens, width = probes.shape
    return pl.pallas_call(
        functools.partial(ahead_kernel, depth // (NZ * NC)),
        out_shape=(
            jax.ShapeDtypeStruct((width, heads), jnp.bfloat16),
            jax.ShapeDtypeStruct((tokens, heads), jnp.float32),
            jax.ShapeDtypeStruct((tokens, depth), jnp.bfloat16),
        ),
        in_specs=[SMEM, VMEM, HBM, VMEM, HBM],
        out_specs=(HBM, VMEM, VMEM),
        scratch_shapes=[
            pltpu.VMEM((tokens, depth), jnp.bfloat16),
            pltpu.SemaphoreType.DMA,
            pltpu.SemaphoreType.DMA((2,)),
        ],
        input_output_aliases={4: 0},
        compiler_params=LIMIT,
        cost_estimate=cost(2 * depth * heads * tokens, 2 * depth * (heads + 2 * tokens)),
    )(place, block, probes, carried[1], carried[0])


def order_sums(sums, rows):
    return pl.pallas_call(
        functools.partial(order_kernel, rows),
        out_shape=jax.ShapeDtypeStruct((sums.size // LANES, LANES), jnp.float32),
        in_specs=[VMEM],
        out_specs=VMEM,
        compiler_params=SMALL,
        cost_estimate=cost(sums.size, 8 * sums.size),
    )(sums)


def last_step(place, own, other, cols, carried, bias):
    tokens, depth = cols.shape
    width, heads = carried[0].shape
    return pl.pallas_call(
        functools.partial(last_kernel, own.shape[0] // NZ),
        out_shape=(
            jax.ShapeDtypeStruct((width, heads), jnp.bfloat16),
            jax.ShapeDtypeStruct((tokens, heads), jnp.bfloat16),
        ),
        in_specs=[SMEM, VMEM, VMEM, VMEM, VMEM, VMEM, HBM],
        out_specs=(HBM, HBM),
        scratch_shapes=[
            pltpu.VMEM((depth, heads), jnp.bfloat16),
            pltpu.VMEM((tokens, heads), jnp.bfloat16),
            pltpu.SemaphoreType.DMA,
            pltpu.SemaphoreType.DMA,
        ],
        input_output_aliases={6: 0},
        compiler_params=SMALL,
        cost_estimate=cost(2 * depth * heads * tokens, 2 * depth * heads),
    )(place, own, other, cols, carried[1], bias.reshape(1, -1), carried[0])


def body(master, key_bias, probe_tokens):
    dp = lax.axis_index("dp")
    core = lax.rem(dp, NC)
    y = lax.div(dp, HI * NC)
    back = lax.rem(y + 1 + 2 * core, NY)
    place = jnp.stack([y, back, lax.rem(back + 2, NY), lax.rem(y + 2, NY), core])

    own_rows = jnp.transpose(master).astype(jnp.bfloat16)
    own_rows, place = lax.optimization_barrier((own_rows, place))
    mine = lax.all_gather(own_rows, AXES, axis=0, tiled=True, axis_index_groups=Z_RINGS)
    back_same = onward(mine)
    mine_other = swap(mine)
    back_other = onward(mine_other)
    far_same = onward(back_same)
    own = own_sums(mine)
    parts = lax.all_to_all(own, "tp", split_axis=0, concat_axis=0, tiled=True)
    s0 = first_step(place, mine, mine_other, probe_tokens)
    totals, block = block_step(place, back_same, back_other, parts)
    ahead = swap(block)
    s1 = back_step(place, block, probe_tokens, s0)
    sums = lax.all_to_all(
        totals, AXES, split_axis=0, concat_axis=0, tiled=True, axis_index_groups=TEAMS
    )
    far_other = swap(far_same)
    *s2, cols_far = ahead_step(place, ahead, probe_tokens, s1)
    weight, probe_keys = last_step(place, far_same, far_other, cols_far, s2, key_bias)
    checksum = order_sums(sums, own_rows.shape[0]).reshape(-1)
    return (weight, probe_keys, checksum)


def solution(mesh):
    placed = (P("tp", ("role", "dp")), P("tp"), P(("role", "dp"), None))
    return jax.shard_map(
        body,
        mesh=mesh,
        in_specs=placed,
        out_specs=(P(None, "tp"), P(("role", "dp"), "tp"), P()),
        check_vma=False,
    )
```

```python
import functools
import itertools

import jax
import jax.numpy as jnp
from jax import lax
from jax.experimental import pallas as pl
from jax.experimental.pallas import tpu as pltpu
from jax.sharding import PartitionSpec as P


AXES = ("role", "tp", "dp")
NX, NY, NZ, NC, LO = 4, 4, 16, 2, 4
HI = NZ // LO
LANES = 128
SAME, BACK, AHEAD, FAR = range(4)
CORE = 4


def index_of(x, y, z, core):
    y, z, core = y % NY, z % NZ, core % NC
    return ((z % LO) * NX + x) * (NY * HI * NC) + (y * HI + z // LO) * NC + core


CHIPS = list(itertools.product(range(NX), range(NY), range(NZ), range(NC)))
Z_RINGS = [
    [index_of(x, y, z, c) for z in range(NZ)]
    for x, y, c in itertools.product(range(NX), range(NY), range(NC))
]


ONWARD = [(index_of(x, y, z, c), index_of(x, y + 2 * c - 1, z, c)) for x, y, z, c in CHIPS]
TEAMS = [
    [index_of(x, y, z, c) for y, c in itertools.product(range(NY), range(NC))]
    for x, z in itertools.product(range(NX), range(NZ))
]
SWAP = [(index_of(x, y, z, c), index_of(x, y, z, c + 1)) for x, y, z, c in CHIPS]


def onward(value):
    return lax.ppermute(value, AXES, ONWARD)


def swap(value):
    return lax.ppermute(value, AXES, SWAP)


def row_of(place, which, lo, span):
    return pl.multiple_of((lo * NY + place[which]) * span, span)


def assemble(core, piece, block, rows):
    span = HI * NC * rows
    for z in range(NZ):
        at = (z % LO) * span + ((z // LO) * NC + core) * rows
        block[pl.ds(pl.multiple_of(at, rows), rows), :] = piece[pl.ds(z * rows, rows), :]


def fetch(place, which, probes, cols, sem):
    span = cols.shape[1] // LO
    gets = []
    for lo in range(LO):
        get = pltpu.make_async_copy(
            probes.at[:, pl.ds(row_of(place, which, lo, span), span)],
            cols.at[:, pl.ds(lo * span, span)],
            sem,
        )
        get.start()
        gets.append(get)
    return gets


def put_rows(place, which, own, other, weight, rows, sem):
    span = HI * NC * rows
    puts = []
    for side, piece in enumerate((own, other)):
        core = place[CORE] if side == 0 else 1 - place[CORE]
        for z in range(NZ):
            at = row_of(place, which, z % LO, span) + ((z // LO) * NC + core) * rows
            put = pltpu.make_async_copy(
                piece.at[pl.ds(z * rows, rows)],
                weight.at[pl.ds(pl.multiple_of(at, rows), rows)],
                sem,
            )
            put.start()
            puts.append(put)
    return puts


def put_block(place, which, block, weight, rows, sem):
    span = HI * NC * rows
    part = NC * rows
    puts = []
    for lo in range(LO):
        for hi in range(HI):
            at = row_of(place, which, lo, span) + hi * part
            put = pltpu.make_async_copy(
                block.at[pl.ds(lo * span + hi * part, part)],
                weight.at[pl.ds(pl.multiple_of(at, part), part)],
                sem,
            )
            put.start()
            puts.append(put)
    return puts


def sums_kernel(own, sums):
    ones = jnp.ones((8, own.shape[1]), own.dtype)
    s = lax.dot_general(
        ones, own[...], (((1,), (1,)), ((), ())), preferred_element_type=jnp.float32
    )
    for copy in range(NX):
        for j in range(s.shape[1] // LANES):
            sums[copy, j : j + 1, :] = s[0:1, j * LANES : (j + 1) * LANES]


def first_kernel(rows, place, own, other, probes, weight, total, cols, block, put_sem, get_sem):
    gets = fetch(place, SAME, probes, cols, get_sem)
    puts = put_rows(place, SAME, own, other, weight, rows, put_sem)
    assemble(place[CORE], own, block, rows)
    assemble(1 - place[CORE], other, block, rows)
    for get in gets:
        get.wait()
    total[...] = jnp.dot(cols[...], block[...], preferred_element_type=jnp.float32)
    for put in puts:
        put.wait()


def back_kernel(rows, place, own, other, probes, parts, total_in, _, weight, total, totals, block, *refs):
    cols_ahead, cols, sums, put_sem, get_sem, sums_sem, ahead_sem = refs
    gets = fetch(place, BACK, probes, cols, get_sem)
    later = fetch(place, AHEAD, probes, cols_ahead, ahead_sem)
    puts = put_rows(place, BACK, own, other, weight, rows, put_sem)
    assemble(place[CORE], own, block, rows)
    assemble(1 - place[CORE], other, block, rows)
    whole = parts[0]
    for x in range(1, NX):
        whole += parts[x]
    for copy in range(sums.shape[0]):
        sums[copy] = whole
    for get in gets:
        get.wait()
    total[...] = total_in[...] + jnp.dot(
        cols[...], block[...], preferred_element_type=jnp.float32
    )
    out = pltpu.make_async_copy(sums, totals, sums_sem)
    out.start()
    for copy in puts + later + [out]:
        copy.wait()


def ahead_kernel(rows, place, block, cols, probes, total_in, _, weight, total, cols_far, put_sem, get_sem):
    later = fetch(place, FAR, probes, cols_far, get_sem)
    puts = put_block(place, AHEAD, block, weight, rows, put_sem)
    total[...] = total_in[...] + jnp.dot(
        cols[...], block[...], preferred_element_type=jnp.float32
    )
    for copy in puts + later:
        copy.wait()


def order_kernel(rows, sums, checksum):
    first_half = lax.broadcasted_iota(jnp.int32, sums.shape[1:], 1) < rows
    for y in range(NY):
        zero, one = sums[y * NC], sums[y * NC + 1]
        lines = (
            jnp.where(first_half, zero, pltpu.roll(one, rows, 1)),
            jnp.where(first_half, pltpu.roll(zero, rows, 1), one),
        )
        for z in range(NZ):
            at = (z % LO * NY + y) * HI + z // LO
            checksum[at : at + 1, :] = lines[z % 2][z // 2 : z // 2 + 1, :]


def last_kernel(rows, place, own, other, cols, total_in, bias, _, weight, keys, block, made, put_sem, keys_sem):
    puts = put_rows(place, FAR, own, other, weight, rows, put_sem)
    assemble(place[CORE], own, block, rows)
    assemble(1 - place[CORE], other, block, rows)
    total = total_in[...] + jnp.dot(cols[...], block[...], preferred_element_type=jnp.float32)
    made[...] = (total + bias[...]).astype(made.dtype)
    for put in puts[: len(puts) // 2]:
        put.wait()
    out = pltpu.make_async_copy(made, keys, keys_sem)
    out.start()
    for copy in puts[len(puts) // 2 :] + [out]:
        copy.wait()


VMEM = pl.BlockSpec(memory_space=pltpu.VMEM)
SMEM = pl.BlockSpec(memory_space=pltpu.SMEM)
HBM = pl.BlockSpec(memory_space=pltpu.HBM)
LIMIT = pltpu.CompilerParams(vmem_limit_bytes=50 << 20)
SMALL = pltpu.CompilerParams(vmem_limit_bytes=16 << 20)


def sizes(piece, probes):
    rows = piece.shape[0] // NZ
    return rows, HI * NC * rows, piece.shape[1], probes.shape[0], probes.shape[1]


def cost(flops, moved):
    return pl.CostEstimate(flops=flops, bytes_accessed=moved, transcendentals=0)


def own_sums(own):
    return pl.pallas_call(
        sums_kernel,
        out_shape=jax.ShapeDtypeStruct((NX, own.shape[0] // LANES, LANES), jnp.float32),
        in_specs=[VMEM],
        out_specs=VMEM,
        compiler_params=SMALL,
        cost_estimate=cost(16 * own.size, 2 * own.size),
    )(own)


def near_scratch(tokens, depth):
    return [
        pltpu.VMEM((tokens, depth), jnp.bfloat16),
        pltpu.SemaphoreType.DMA,
        pltpu.SemaphoreType.DMA,
    ]


def first_step(place, own, other, probes):
    rows, span, heads, tokens, width = sizes(own, probes)
    depth = LO * span
    cols, put_sem, get_sem = near_scratch(tokens, depth)
    return pl.pallas_call(
        functools.partial(first_kernel, rows),
        out_shape=(
            jax.ShapeDtypeStruct((width, heads), jnp.bfloat16),
            jax.ShapeDtypeStruct((tokens, heads), jnp.float32),
        ),
        in_specs=[SMEM, VMEM, VMEM, HBM],
        out_specs=(HBM, VMEM),
        scratch_shapes=[cols, pltpu.VMEM((depth, heads), jnp.bfloat16), put_sem, get_sem],
        compiler_params=LIMIT,
        cost_estimate=cost(2 * depth * heads * tokens, 2 * depth * (heads + tokens)),
    )(place, own, other, probes)


def back_step(place, own, other, probes, parts, carried):
    rows, span, heads, tokens, width = sizes(own, probes)
    depth = LO * span
    cols, put_sem, get_sem = near_scratch(tokens, depth)
    return pl.pallas_call(
        functools.partial(back_kernel, rows),
        out_shape=(
            jax.ShapeDtypeStruct((width, heads), jnp.bfloat16),
            jax.ShapeDtypeStruct((tokens, heads), jnp.float32),
            jax.ShapeDtypeStruct((NY * NC, *parts.shape[1:]), jnp.float32),
            jax.ShapeDtypeStruct((depth, heads), jnp.bfloat16),
            jax.ShapeDtypeStruct((tokens, depth), jnp.bfloat16),
        ),
        in_specs=[SMEM, VMEM, VMEM, HBM, VMEM, VMEM, HBM],
        out_specs=(HBM, VMEM, HBM, VMEM, VMEM),
        scratch_shapes=[
            cols,
            pltpu.VMEM((NY * NC, *parts.shape[1:]), jnp.float32),
            put_sem,
            get_sem,
            pltpu.SemaphoreType.DMA,
            pltpu.SemaphoreType.DMA,
        ],
        input_output_aliases={6: 0},
        compiler_params=LIMIT,
        cost_estimate=cost(2 * depth * heads * tokens, 2 * depth * (heads + 2 * tokens)),
    )(place, own, other, probes, parts, carried[1], carried[0])


def ahead_step(place, block, cols, probes, carried):
    depth, heads = block.shape
    tokens, width = probes.shape
    return pl.pallas_call(
        functools.partial(ahead_kernel, depth // (NZ * NC)),
        out_shape=(
            jax.ShapeDtypeStruct((width, heads), jnp.bfloat16),
            jax.ShapeDtypeStruct((tokens, heads), jnp.float32),
            jax.ShapeDtypeStruct((tokens, depth), jnp.bfloat16),
        ),
        in_specs=[SMEM, VMEM, VMEM, HBM, VMEM, HBM],
        out_specs=(HBM, VMEM, VMEM),
        scratch_shapes=[
            pltpu.SemaphoreType.DMA,
            pltpu.SemaphoreType.DMA,
        ],
        input_output_aliases={5: 0},
        compiler_params=LIMIT,
        cost_estimate=cost(2 * depth * heads * tokens, 2 * depth * (heads + tokens)),
    )(place, block, cols, probes, carried[1], carried[0])


def order_sums(sums, rows):
    return pl.pallas_call(
        functools.partial(order_kernel, rows),
        out_shape=jax.ShapeDtypeStruct((sums.size // LANES, LANES), jnp.float32),
        in_specs=[VMEM],
        out_specs=VMEM,
        compiler_params=SMALL,
        cost_estimate=cost(sums.size, 8 * sums.size),
    )(sums)


def last_step(place, own, other, cols, carried, bias):
    tokens, depth = cols.shape
    width, heads = carried[0].shape
    return pl.pallas_call(
        functools.partial(last_kernel, own.shape[0] // NZ),
        out_shape=(
            jax.ShapeDtypeStruct((width, heads), jnp.bfloat16),
            jax.ShapeDtypeStruct((tokens, heads), jnp.bfloat16),
        ),
        in_specs=[SMEM, VMEM, VMEM, VMEM, VMEM, VMEM, HBM],
        out_specs=(HBM, HBM),
        scratch_shapes=[
            pltpu.VMEM((depth, heads), jnp.bfloat16),
            pltpu.VMEM((tokens, heads), jnp.bfloat16),
            pltpu.SemaphoreType.DMA,
            pltpu.SemaphoreType.DMA,
        ],
        input_output_aliases={6: 0},
        compiler_params=SMALL,
        cost_estimate=cost(2 * depth * heads * tokens, 2 * depth * heads),
    )(place, own, other, cols, carried[1], bias.reshape(1, -1), carried[0])


def body(master, key_bias, probe_tokens):
    dp = lax.axis_index("dp")
    core = lax.rem(dp, NC)
    y = lax.div(dp, HI * NC)
    back = lax.rem(y + 1 + 2 * core, NY)
    place = jnp.stack([y, back, lax.rem(back + 2, NY), lax.rem(y + 2, NY), core])

    own_rows = jnp.transpose(master).astype(jnp.bfloat16)
    own_rows, place = lax.optimization_barrier((own_rows, place))
    mine = lax.all_gather(own_rows, AXES, axis=0, tiled=True, axis_index_groups=Z_RINGS)
    back_same = onward(mine)
    mine_other = swap(mine)
    back_other = onward(mine_other)
    far_same = onward(back_same)
    own = own_sums(mine)
    parts = lax.all_to_all(own, "tp", split_axis=0, concat_axis=0, tiled=True)
    s0 = first_step(place, mine, mine_other, probe_tokens)
    *s1, totals, block, cols_ahead = back_step(
        place, back_same, back_other, probe_tokens, parts, s0
    )
    ahead = swap(block)
    sums = lax.all_to_all(
        totals, AXES, split_axis=0, concat_axis=0, tiled=True, axis_index_groups=TEAMS
    )
    far_other = swap(far_same)
    *s2, cols_far = ahead_step(place, ahead, cols_ahead, probe_tokens, s1)
    weight, probe_keys = last_step(place, far_same, far_other, cols_far, s2, key_bias)
    checksum = order_sums(sums, own_rows.shape[0]).reshape(-1)
    return (weight, probe_keys, checksum)


def solution(mesh):
    placed = (P("tp", ("role", "dp")), P("tp"), P(("role", "dp"), None))
    return jax.shard_map(
        body,
        mesh=mesh,
        in_specs=placed,
        out_specs=(P(None, "tp"), P(("role", "dp"), "tp"), P()),
        check_vma=False,
    )
```

```python
import functools
import itertools

import jax
import jax.numpy as jnp
from jax import lax
from jax.experimental import pallas as pl
from jax.experimental.pallas import tpu as pltpu
from jax.sharding import PartitionSpec as P


AXES = ("role", "tp", "dp")
NX, NY, NZ, NC, LO = 4, 4, 16, 2, 4
HI = NZ // LO
LANES = 128
SAME, BACK, AHEAD, FAR = range(4)
CORE = 4


def index_of(x, y, z, core):
    y, z, core = y % NY, z % NZ, core % NC
    return ((z % LO) * NX + x) * (NY * HI * NC) + (y * HI + z // LO) * NC + core


CHIPS = list(itertools.product(range(NX), range(NY), range(NZ), range(NC)))
Z_RINGS = [
    [index_of(x, y, z, c) for z in range(NZ)]
    for x, y, c in itertools.product(range(NX), range(NY), range(NC))
]


ONWARD = [(index_of(x, y, z, c), index_of(x, y + 2 * c - 1, z, c)) for x, y, z, c in CHIPS]
TEAMS = [
    [index_of(x, y, z, c) for y, c in itertools.product(range(NY), range(NC))]
    for x, z in itertools.product(range(NX), range(NZ))
]
SWAP = [(index_of(x, y, z, c), index_of(x, y, z, c + 1)) for x, y, z, c in CHIPS]


def onward(value):
    return lax.ppermute(value, AXES, ONWARD)


def swap(value):
    return lax.ppermute(value, AXES, SWAP)


def row_of(place, which, lo, span):
    return pl.multiple_of((lo * NY + place[which]) * span, span)


def assemble(core, piece, block, rows):
    span = HI * NC * rows
    for z in range(NZ):
        at = (z % LO) * span + ((z // LO) * NC + core) * rows
        block[pl.ds(pl.multiple_of(at, rows), rows), :] = piece[pl.ds(z * rows, rows), :]


def fetch(place, which, probes, cols, sem):
    span = cols.shape[1] // LO
    gets = []
    for lo in range(LO):
        get = pltpu.make_async_copy(
            probes.at[:, pl.ds(row_of(place, which, lo, span), span)],
            cols.at[:, pl.ds(lo * span, span)],
            sem,
        )
        get.start()
        gets.append(get)
    return gets


def put_rows(place, which, own, other, weight, rows, sem):
    span = HI * NC * rows
    puts = []
    for side, piece in enumerate((own, other)):
        core = place[CORE] if side == 0 else 1 - place[CORE]
        for z in range(NZ):
            at = row_of(place, which, z % LO, span) + ((z // LO) * NC + core) * rows
            put = pltpu.make_async_copy(
                piece.at[pl.ds(z * rows, rows)],
                weight.at[pl.ds(pl.multiple_of(at, rows), rows)],
                sem,
            )
            put.start()
            puts.append(put)
    return puts


def put_block(place, which, block, weight, rows, sem):
    span = HI * NC * rows
    part = NC * rows
    puts = []
    for lo in range(LO):
        for hi in range(HI):
            at = row_of(place, which, lo, span) + hi * part
            put = pltpu.make_async_copy(
                block.at[pl.ds(lo * span + hi * part, part)],
                weight.at[pl.ds(pl.multiple_of(at, part), part)],
                sem,
            )
            put.start()
            puts.append(put)
    return puts


def sums_kernel(own, sums):
    ones = jnp.ones((8, own.shape[1]), own.dtype)
    s = lax.dot_general(
        ones, own[...], (((1,), (1,)), ((), ())), preferred_element_type=jnp.float32
    )
    for copy in range(NX):
        for j in range(s.shape[1] // LANES):
            sums[copy, j : j + 1, :] = s[0:1, j * LANES : (j + 1) * LANES]


def first_kernel(rows, place, own, other, probes, weight, total, cols, block, put_sem, get_sem):
    gets = fetch(place, SAME, probes, cols, get_sem)
    puts = put_rows(place, SAME, own, other, weight, rows, put_sem)
    assemble(place[CORE], own, block, rows)
    assemble(1 - place[CORE], other, block, rows)
    for get in gets:
        get.wait()
    total[...] = jnp.dot(cols[...], block[...], preferred_element_type=jnp.float32)
    for put in puts:
        put.wait()


def back_kernel(rows, place, own, other, probes, parts, total_in, _, weight, total, totals, block, *refs):
    cols, sums, put_sem, get_sem, sums_sem = refs
    gets = fetch(place, BACK, probes, cols, get_sem)
    puts = put_rows(place, BACK, own, other, weight, rows, put_sem)
    assemble(place[CORE], own, block, rows)
    assemble(1 - place[CORE], other, block, rows)
    whole = parts[0]
    for x in range(1, NX):
        whole += parts[x]
    for copy in range(sums.shape[0]):
        sums[copy] = whole
    for get in gets:
        get.wait()
    total[...] = total_in[...] + jnp.dot(
        cols[...], block[...], preferred_element_type=jnp.float32
    )
    out = pltpu.make_async_copy(sums, totals, sums_sem)
    out.start()
    for put in puts:
        put.wait()
    out.wait()


def ahead_kernel(rows, place, block, probes, total_in, _, weight, total, cols_far, cols, put_sem, get_sem):
    gets = fetch(place, AHEAD, probes, cols, get_sem.at[0])
    later = fetch(place, FAR, probes, cols_far, get_sem.at[1])
    puts = put_block(place, AHEAD, block, weight, rows, put_sem)
    for get in gets:
        get.wait()
    total[...] = total_in[...] + jnp.dot(
        cols[...], block[...], preferred_element_type=jnp.float32
    )
    for copy in puts + later:
        copy.wait()


def order_kernel(rows, sums, checksum):
    first_half = lax.broadcasted_iota(jnp.int32, sums.shape[1:], 1) < rows
    for y in range(NY):
        zero, one = sums[y * NC], sums[y * NC + 1]
        lines = (
            jnp.where(first_half, zero, pltpu.roll(one, rows, 1)),
            jnp.where(first_half, pltpu.roll(zero, rows, 1), one),
        )
        for z in range(NZ):
            at = (z % LO * NY + y) * HI + z // LO
            checksum[at : at + 1, :] = lines[z % 2][z // 2 : z // 2 + 1, :]


def last_kernel(rows, place, own, other, cols, total_in, bias, _, weight, keys, block, made, put_sem, keys_sem):
    puts = put_rows(place, FAR, own, other, weight, rows, put_sem)
    assemble(place[CORE], own, block, rows)
    assemble(1 - place[CORE], other, block, rows)
    total = total_in[...] + jnp.dot(cols[...], block[...], preferred_element_type=jnp.float32)
    made[...] = (total + bias[...]).astype(made.dtype)
    for put in puts[: len(puts) // 2]:
        put.wait()
    out = pltpu.make_async_copy(made, keys, keys_sem)
    out.start()
    for copy in puts[len(puts) // 2 :] + [out]:
        copy.wait()


VMEM = pl.BlockSpec(memory_space=pltpu.VMEM)
SMEM = pl.BlockSpec(memory_space=pltpu.SMEM)
HBM = pl.BlockSpec(memory_space=pltpu.HBM)
LIMIT = pltpu.CompilerParams(vmem_limit_bytes=50 << 20)
SMALL = pltpu.CompilerParams(vmem_limit_bytes=16 << 20)


def sizes(piece, probes):
    rows = piece.shape[0] // NZ
    return rows, HI * NC * rows, piece.shape[1], probes.shape[0], probes.shape[1]


def cost(flops, moved):
    return pl.CostEstimate(flops=flops, bytes_accessed=moved, transcendentals=0)


def own_sums(own):
    return pl.pallas_call(
        sums_kernel,
        out_shape=jax.ShapeDtypeStruct((NX, own.shape[0] // LANES, LANES), jnp.float32),
        in_specs=[VMEM],
        out_specs=VMEM,
        compiler_params=SMALL,
        cost_estimate=cost(16 * own.size, 2 * own.size),
    )(own)


def near_scratch(tokens, depth):
    return [
        pltpu.VMEM((tokens, depth), jnp.bfloat16),
        pltpu.SemaphoreType.DMA,
        pltpu.SemaphoreType.DMA,
    ]


def first_step(place, own, other, probes):
    rows, span, heads, tokens, width = sizes(own, probes)
    depth = LO * span
    cols, put_sem, get_sem = near_scratch(tokens, depth)
    return pl.pallas_call(
        functools.partial(first_kernel, rows),
        out_shape=(
            jax.ShapeDtypeStruct((width, heads), jnp.bfloat16),
            jax.ShapeDtypeStruct((tokens, heads), jnp.float32),
        ),
        in_specs=[SMEM, VMEM, VMEM, HBM],
        out_specs=(HBM, VMEM),
        scratch_shapes=[cols, pltpu.VMEM((depth, heads), jnp.bfloat16), put_sem, get_sem],
        compiler_params=LIMIT,
        cost_estimate=cost(2 * depth * heads * tokens, 2 * depth * (heads + tokens)),
    )(place, own, other, probes)


def back_step(place, own, other, probes, parts, carried):
    rows, span, heads, tokens, width = sizes(own, probes)
    depth = LO * span
    cols, put_sem, get_sem = near_scratch(tokens, depth)
    return pl.pallas_call(
        functools.partial(back_kernel, rows),
        out_shape=(
            jax.ShapeDtypeStruct((width, heads), jnp.bfloat16),
            jax.ShapeDtypeStruct((tokens, heads), jnp.float32),
            jax.ShapeDtypeStruct((NY * NC, *parts.shape[1:]), jnp.float32),
            jax.ShapeDtypeStruct((depth, heads), jnp.bfloat16),
        ),
        in_specs=[SMEM, VMEM, VMEM, HBM, VMEM, VMEM, HBM],
        out_specs=(HBM, VMEM, HBM, VMEM),
        scratch_shapes=[
            cols,
            pltpu.VMEM((NY * NC, *parts.shape[1:]), jnp.float32),
            put_sem,
            get_sem,
            pltpu.SemaphoreType.DMA,
        ],
        input_output_aliases={6: 0},
        compiler_params=LIMIT,
        cost_estimate=cost(2 * depth * heads * tokens, 2 * depth * (heads + tokens)),
    )(place, own, other, probes, parts, carried[1], carried[0])


def ahead_step(place, block, probes, carried):
    depth, heads = block.shape
    tokens, width = probes.shape
    return pl.pallas_call(
        functools.partial(ahead_kernel, depth // (NZ * NC)),
        out_shape=(
            jax.ShapeDtypeStruct((width, heads), jnp.bfloat16),
            jax.ShapeDtypeStruct((tokens, heads), jnp.float32),
            jax.ShapeDtypeStruct((tokens, depth), jnp.bfloat16),
        ),
        in_specs=[SMEM, VMEM, HBM, VMEM, HBM],
        out_specs=(HBM, VMEM, VMEM),
        scratch_shapes=[
            pltpu.VMEM((tokens, depth), jnp.bfloat16),
            pltpu.SemaphoreType.DMA,
            pltpu.SemaphoreType.DMA((2,)),
        ],
        input_output_aliases={4: 0},
        compiler_params=LIMIT,
        cost_estimate=cost(2 * depth * heads * tokens, 2 * depth * (heads + 2 * tokens)),
    )(place, block, probes, carried[1], carried[0])


def order_sums(sums, rows):
    return pl.pallas_call(
        functools.partial(order_kernel, rows),
        out_shape=jax.ShapeDtypeStruct((sums.size // LANES, LANES), jnp.float32),
        in_specs=[VMEM],
        out_specs=VMEM,
        compiler_params=SMALL,
        cost_estimate=cost(sums.size, 8 * sums.size),
    )(sums)


def last_step(place, own, other, cols, carried, bias):
    tokens, depth = cols.shape
    width, heads = carried[0].shape
    return pl.pallas_call(
        functools.partial(last_kernel, own.shape[0] // NZ),
        out_shape=(
            jax.ShapeDtypeStruct((width, heads), jnp.bfloat16),
            jax.ShapeDtypeStruct((tokens, heads), jnp.bfloat16),
        ),
        in_specs=[SMEM, VMEM, VMEM, VMEM, VMEM, VMEM, HBM],
        out_specs=(HBM, HBM),
        scratch_shapes=[
            pltpu.VMEM((depth, heads), jnp.bfloat16),
            pltpu.VMEM((tokens, heads), jnp.bfloat16),
            pltpu.SemaphoreType.DMA,
            pltpu.SemaphoreType.DMA,
        ],
        input_output_aliases={6: 0},
        compiler_params=SMALL,
        cost_estimate=cost(2 * depth * heads * tokens, 2 * depth * heads),
    )(place, own, other, cols, carried[1], bias.reshape(1, -1), carried[0])


def body(master, key_bias, probe_tokens):
    dp = lax.axis_index("dp")
    core = lax.rem(dp, NC)
    y = lax.div(dp, HI * NC)
    back = lax.rem(y + 1 + 2 * core, NY)
    place = jnp.stack([y, back, lax.rem(back + 2, NY), lax.rem(y + 2, NY), core])

    own_rows = jnp.transpose(master).astype(jnp.bfloat16)
    own_rows, place = lax.optimization_barrier((own_rows, place))
    mine = lax.all_gather(own_rows, AXES, axis=0, tiled=True, axis_index_groups=Z_RINGS)
    back_same = onward(mine)
    mine_other = swap(mine)
    back_other = onward(mine_other)
    far_same = onward(back_same)
    own = own_sums(mine)
    parts = lax.all_to_all(own, "tp", split_axis=0, concat_axis=0, tiled=True)
    s0 = first_step(place, mine, mine_other, probe_tokens)
    *s1, totals, block = back_step(
        place, back_same, back_other, probe_tokens, parts, s0
    )
    ahead = swap(block)
    sums = lax.all_to_all(
        totals, AXES, split_axis=0, concat_axis=0, tiled=True, axis_index_groups=TEAMS
    )
    far_other = swap(far_same)
    *s2, cols_far = ahead_step(place, ahead, probe_tokens, s1)
    weight, probe_keys = last_step(place, far_same, far_other, cols_far, s2, key_bias)
    checksum = order_sums(sums, own_rows.shape[0]).reshape(-1)
    return (weight, probe_keys, checksum)


def solution(mesh):
    placed = (P("tp", ("role", "dp")), P("tp"), P(("role", "dp"), None))
    return jax.shard_map(
        body,
        mesh=mesh,
        in_specs=placed,
        out_specs=(P(None, "tp"), P(("role", "dp"), "tp"), P()),
        check_vma=False,
    )
```
